32 devices in a mesh: group: 4 (over y, x), member: 8 (over z, core).
Axes of the slice: x: 2, y: 2, z: 4, core: 2. Of those that a mesh axis runs over, the one named last changes fastest.
Arguments:
- amplitudes: bfloat16 [512, 128, 128], P(('group', 'member')), may hold values from -6 to 6
- integrals: bfloat16 [256, 128, 128], P(('group', 'member')), may hold values from -0.02734375 to 0.02734375
- tasks: int32 [12288, 3], P(('group', 'member')), may hold values from 0 to 15, as said below
- requests: int32 [128, 4], P(('group', 'member')), may hold values from 0 to 7
- counts: int32 [32], P(('group', 'member')), may hold values from 1 to 384, as said below
Outputs:
- residual: float32 [32, 128, 128], P(('group', 'member'))
The draws below stay inside these ranges and needn't reach their ends.
Inputs may be any that keep to these rules, and one draw needn't show every extreme that they name: `tasks`: column 0 is below 16, column 1 below 16, column 2 below 8; slots beyond a device's count hold valid entries too. `counts`: some device has 384 live tasks in every draw.
All inputs are finite; a program needn't handle non-finite values.
Results may differ from the reference program's by a relative error of at most 0.0003.
Values may be sent and summed in bfloat16 or wider, within the bound.
A program may use at most 64 MiB of HBM per device.

```python
import jax
import jax.numpy as jnp
from jax import lax

TILE = 128
AMP_DEV = 16
V_DEV = 8
FETCH_CAP = 4
TASK_CAP = 384
FETCH_SLOTS = 16
RES_GROUP = 8
AMPS = 512
VTILES = 256
TASKS = 12288
REQ_ROWS = 128
RTILES = 32
N_GROUP = 4
N_MEMBER = 8
DEVICES = 32


def draw_tasks(key, part):
    first = jax.random.randint(jax.random.fold_in(key, 11), (TASKS,), 0, AMP_DEV)
    second = jax.random.randint(jax.random.fold_in(key, 12), (TASKS,), 0, FETCH_SLOTS)
    third = jax.random.randint(jax.random.fold_in(key, 13), (TASKS,), 0, RES_GROUP)
    return jnp.stack([first, second, third], axis=1).astype(jnp.int32)


def draw_counts(key, part):
    shifts = jax.random.randint(jax.random.fold_in(key, 21), (DEVICES,), 0, 4)
    base = jnp.right_shift(jnp.full((DEVICES,), TASK_CAP, jnp.int32), shifts.astype(jnp.int32))
    jitter = jax.random.randint(jax.random.fold_in(key, 22), (DEVICES,), 0, base // 2 + 1)
    values = base - jitter
    chosen = jax.random.randint(jax.random.fold_in(key, 23), (), 0, DEVICES)
    values = jnp.where(jnp.arange(DEVICES) == chosen, TASK_CAP, values)
    return values.astype(jnp.int32)


def plant(entries, rng, low, high):
    longest = entries.shape.index(max(entries.shape))
    spots = []
    for shift in (0, 1):
        where = [jax.random.randint(jax.random.fold_in(rng, axis), (), 0, length) for axis, length in enumerate(entries.shape)]
        where[longest] = (where[longest] + shift) % entries.shape[longest]
        spots.append(tuple(where))
    return entries.at[spots[0]].set(low).at[spots[1]].set(high)


def block_scale(key, shape, pieces, smallest, largest):
    loudness = 1.0
    for axis_at, shards_of in pieces:
        steps = jax.random.uniform(jax.random.fold_in(jax.random.fold_in(key, 6), axis_at), (shards_of,), jnp.float32, smallest / len(pieces), largest / len(pieces))
        loudness = loudness * jnp.repeat(jnp.exp(steps), shape[axis_at] // shards_of).reshape((-1,) + (1,) * (len(shape) - 1 - axis_at))
    return loudness


def noise(key, dims, scale, most, pieces=(), kind=jnp.bfloat16):
    values = scale * jax.random.normal(key, dims, jnp.float32)
    if pieces:
        values = values * block_scale(key, dims, pieces, -0.22, 0.18)
    return jnp.clip(values, -most, most).astype(kind)


def setup_inputs(seed: int = 0) -> dict:
    keys = jax.random.split(jax.random.key(seed), 6)
    return {
        "amplitudes": noise(keys[0], (AMPS, TILE, TILE), 1.0, 6.0, ((0, 32),)),
        "integrals": noise(keys[1], (VTILES, TILE, TILE), (TILE * TASK_CAP) ** -0.5, 0.02734375, ((0, 32),)),
        "tasks": draw_tasks(jax.random.fold_in(keys[5], 71), 0),
        "requests": plant(jax.random.randint(keys[3], (REQ_ROWS, FETCH_CAP), 0, V_DEV), jax.random.fold_in(keys[3], 1), 0, V_DEV - 1).astype(jnp.int32),
        "counts": draw_counts(jax.random.fold_in(keys[5], 71), 0),
    }


def reference(amplitudes, integrals, tasks, requests, counts):
    tile = amplitudes.shape[1]

    def device(d, result):
        d = jnp.asarray(d).astype(jnp.int32)
        group_index = d // N_MEMBER
        member_index = d % N_MEMBER
        amps = lax.dynamic_slice_in_dim(amplitudes, d * AMP_DEV, AMP_DEV, 0)
        wanted = lax.dynamic_slice_in_dim(requests, d * N_GROUP, N_GROUP, 0)
        column = jnp.arange(N_GROUP, dtype=jnp.int32)[:, None] * N_MEMBER + member_index
        index = ((column * V_DEV + wanted).reshape(-1)).astype(jnp.int32)
        fetched = integrals[index]
        own = lax.dynamic_slice_in_dim(tasks, d * TASK_CAP, TASK_CAP, 0)
        count = counts[d]

        def block(k, total):
            start = (jnp.asarray(k) * 16).astype(jnp.int32)
            rows = lax.dynamic_slice_in_dim(own, start, 16, 0)
            valid = (start + jnp.arange(16, dtype=jnp.int32)) < count
            left = amps[rows[:, 0]].astype(jnp.float32)
            right = fetched[rows[:, 1]].astype(jnp.float32)
            product = jnp.einsum("kij,kjl->kil", left, right)
            product = jnp.where(valid[:, None, None], product, jnp.zeros_like(product))
            target = (group_index * RES_GROUP + rows[:, 2]).astype(jnp.int32)
            return total.at[target].add(product)

        return lax.fori_loop(0, (count + 15) // 16, block, result)

    start_total = jnp.zeros((RTILES, tile, tile), jnp.float32)
    return lax.fori_loop(0, DEVICES, device, start_total)
```

```python
import functools

import jax
import jax.numpy as jnp
from jax import lax
from jax.experimental import pallas as pl
from jax.experimental.pallas import tpu as pltpu
from jax.sharding import PartitionSpec as P

RES_DEV = 1
BLOCK = 8
UNROLL = 8
MESH = pl.DeviceIdType.MESH


def round_up(n, k):
    return (n + k - 1) // k * k


def sort_tasks(n_res, n_blocks, n_amps, n_fetched, count, task_ref, slot_ref, last_ref):
    cap = task_ref.shape[1]
    slots = slot_ref.shape[1]
    valid = lax.broadcasted_iota(jnp.int32, (n_res, cap), 1) < count
    rows = lax.broadcasted_iota(jnp.int32, (n_res, cap), 0)
    hit = jnp.where(valid & (rows == task_ref[2:3, :]), 1.0, 0.0)
    upper = jnp.where(
        lax.broadcasted_iota(jnp.int32, (cap, cap), 0) <= lax.broadcasted_iota(jnp.int32, (cap, cap), 1), 1.0, 0.0
    ).astype(jnp.bfloat16)
    rank = jnp.dot(hit.astype(jnp.bfloat16), upper, preferred_element_type=jnp.float32)
    number = jnp.sum(hit, axis=1, keepdims=True).astype(jnp.int32)
    blocks = jnp.maximum((number + (BLOCK - 1)) // BLOCK, 1)
    blocks = jnp.broadcast_to(blocks, (n_res, 128))
    lower = jnp.where(
        lax.broadcasted_iota(jnp.int32, (n_res, n_res), 1) < lax.broadcasted_iota(jnp.int32, (n_res, n_res), 0), 1.0, 0.0
    ).astype(jnp.bfloat16)
    first = jnp.dot(
        lower, blocks.astype(jnp.float32).astype(jnp.bfloat16), preferred_element_type=jnp.float32
    ).astype(jnp.int32)
    last_ref[...] = jnp.clip(first + blocks - 1, 0, n_blocks - 1)
    place = jnp.sum(hit * (rank + (first[:, :1] * BLOCK).astype(jnp.float32)), axis=0, keepdims=True) - 1.0
    place = place.astype(jnp.int32)
    chosen = jnp.where(lax.broadcasted_iota(jnp.int32, (slots, cap), 0) == place, 1.0, 0.0).astype(jnp.bfloat16)
    line = lax.broadcasted_iota(jnp.int32, (8, cap), 0)
    values = jnp.where(line == 0, task_ref[0:1, :] + 1, jnp.where(line == 1, task_ref[1:2, :], 0))
    picked = lax.dot_general(
        values.astype(jnp.float32).astype(jnp.bfloat16),
        chosen,
        (((1,), (1,)), ((), ())),
        preferred_element_type=jnp.float32,
    ).astype(jnp.int32)
    starts = jnp.sum(jnp.where(lax.broadcasted_iota(jnp.int32, (n_res, 128), 1) == first, 1, 0), axis=0, keepdims=True)
    keep = jnp.concatenate([1 - starts, jnp.zeros((1, slots - 128), jnp.int32)], axis=1)
    picked = jnp.clip(picked, 0, jnp.where(lax.broadcasted_iota(jnp.int32, (8, slots), 0) == 0, n_amps, n_fetched - 1))
    slot_ref[...] = jnp.where(lax.broadcasted_iota(jnp.int32, (8, slots), 0) == 2, keep, picked)


def main_kernel(
    n_group, n_member, n_blocks,
    request_hbm, task_hbm, count_hbm, amp_hbm, int_hbm, out_ref,
    request_ref, task_ref, count_ref, slot_vmem, last_vmem, slot_ref, last_ref, amps, ints, fetched, outgoing, wanted, running, half, half_in, pair, pair_in,
    local_sem, req_send, req_recv, tile_send, tile_recv, half_send, half_recv, pair_send, pair_recv,
):
    g = lax.axis_index("group")
    m = lax.axis_index("member")
    n_z = n_member // 2
    z, core = m // 2, m % 2
    fetch_cap = request_ref.shape[1]
    tile = amps.shape[1]
    amp_copy = pltpu.make_async_copy(amp_hbm, amps.at[pl.ds(1, amp_hbm.shape[0])], local_sem.at[0])
    int_copy = pltpu.make_async_copy(int_hbm, ints, local_sem.at[1])
    request_copy = pltpu.make_async_copy(request_hbm, request_ref, local_sem.at[2])
    task_copy = pltpu.make_async_copy(task_hbm, task_ref, local_sem.at[3])
    count_copy = pltpu.make_async_copy(count_hbm, count_ref, local_sem.at[4])
    for copy in (request_copy, int_copy, task_copy, count_copy, amp_copy):
        copy.start()
    group_peers = [((g + i) % n_group, m) for i in range(1, n_group)]
    sibling = (g, z * 2 + 1 - core)
    z_peers = [(g, ((z + i) % n_z) * 2 + core) for i in range(1, n_z)]

    barrier = pltpu.get_barrier_semaphore()
    for peer in group_peers + [sibling] + z_peers:
        pl.semaphore_signal(barrier, inc=1, device_id=peer, device_id_type=MESH)
    amps[0] = jnp.zeros((tile, tile), amps.dtype)
    request_copy.wait()
    pl.semaphore_wait(barrier, n_group + n_z - 1)

    asks = []
    for i, peer in enumerate(group_peers):
        ask = pltpu.make_async_remote_copy(
            src_ref=request_ref, dst_ref=wanted.at[i], send_sem=req_send.at[i], recv_sem=req_recv.at[i],
            device_id=peer, device_id_type=MESH,
        )
        ask.start()
        asks.append(ask)
    int_copy.wait()
    for c in range(fetch_cap):
        fetched[g * fetch_cap + c] = ints[request_ref[g, c]]
    sends = []
    for i in range(n_group - 1):
        asks[i].wait_recv()
        for c in range(fetch_cap):
            outgoing[i, c] = ints[wanted[i, g, c]]
        send = pltpu.make_async_remote_copy(
            src_ref=outgoing.at[i], dst_ref=fetched.at[pl.ds(g * fetch_cap, fetch_cap)],
            send_sem=tile_send.at[i], recv_sem=tile_recv.at[i],
            device_id=((g + n_group - i - 1) % n_group, m), device_id_type=MESH,
        )
        send.start()
        sends.append(send)
    count_copy.wait()
    task_copy.wait()
    sort_tasks(
        n_member * RES_DEV, n_blocks, amp_hbm.shape[0], fetched.shape[0], count_ref[0], task_ref, slot_vmem, last_vmem,
    )
    slot_copy = pltpu.make_async_copy(slot_vmem, slot_ref, local_sem.at[5])
    last_copy = pltpu.make_async_copy(last_vmem, last_ref, local_sem.at[6])
    slot_copy.start()
    last_copy.start()
    amp_copy.wait()
    slot_copy.wait()
    last_copy.wait()
    for i in range(n_group - 1):
        asks[i].wait_send()
        source = (g + i + 1) % n_group
        pltpu.make_async_remote_copy(
            src_ref=outgoing.at[i], dst_ref=fetched.at[pl.ds(source * fetch_cap, fetch_cap)],
            send_sem=tile_send.at[i], recv_sem=tile_recv.at[i],
            device_id=group_peers[i], device_id_type=MESH,
        ).wait_recv()

    def block(b, total):
        for u in range(UNROLL):
            total = one_block(b * UNROLL + u, total)
        return total

    def one_block(b, total):
        left = []
        right = []
        for t in range(BLOCK):
            left.append(amps[slot_ref[0, b * BLOCK + t]])
            right.append(fetched[slot_ref[1, b * BLOCK + t]])
        product = jnp.dot(
            jnp.concatenate(left, axis=1), jnp.concatenate(right, axis=0), preferred_element_type=jnp.float32
        )
        total = jnp.where(slot_ref[2, b] != 0, total, 0.0) + product
        running[b] = total
        return total

    lax.fori_loop(0, n_blocks // UNROLL, block, jnp.zeros((tile, tile), jnp.float32))

    for k in range(n_z):
        half[k] = running[last_ref[2 * k + 1 - core, 0]]
    swap = pltpu.make_async_remote_copy(
        src_ref=half, dst_ref=half_in, send_sem=half_send, recv_sem=half_recv,
        device_id=sibling, device_id_type=MESH,
    )
    swap.start()
    swap.wait_recv()
    parts = []
    for i in range(1, n_z):
        k = (z + i) % n_z
        pair[i - 1] = running[last_ref[2 * k + core, 0]] + half_in[k]
        part = pltpu.make_async_remote_copy(
            src_ref=pair.at[i - 1], dst_ref=pair_in.at[i - 1],
            send_sem=pair_send.at[i - 1], recv_sem=pair_recv.at[i - 1],
            device_id=z_peers[i - 1], device_id_type=MESH,
        )
        part.start()
        parts.append(part)
    result = running[last_ref[m, 0]] + half_in[z]
    for i in range(n_z - 1):
        parts[i].wait_recv()
        result = result + pair_in[i]
    out_ref[0] = result
    swap.wait_send()
    for copy in sends + parts:
        copy.wait_send()


def sorted_tasks_call(amplitudes, integrals, tasks, requests, counts):
    tile = amplitudes.shape[1]
    n_group = lax.axis_size("group")
    n_member = lax.axis_size("member")
    n_res = RES_DEV * n_member
    cap = tasks.shape[0]
    fetch_cap = requests.shape[1]
    n_z = n_member // 2
    n_blocks = round_up((cap + BLOCK - 1) // BLOCK + n_res, UNROLL)
    slots = round_up(n_blocks * BLOCK, 128)
    vmem = pl.BlockSpec(memory_space=pltpu.VMEM)
    hbm = pl.BlockSpec(memory_space=pltpu.HBM)
    f32, bf16 = jnp.float32, amplitudes.dtype
    dma = pltpu.SemaphoreType.DMA
    return pl.pallas_call(
        functools.partial(main_kernel, n_group, n_member, n_blocks),
        out_shape=jax.ShapeDtypeStruct((RES_DEV, tile, tile), f32),
        in_specs=[hbm] * 5,
        out_specs=vmem,
        scratch_shapes=[
            pltpu.SMEM(requests.shape, jnp.int32),
            pltpu.VMEM((tasks.shape[1], cap), jnp.int32),
            pltpu.SMEM(counts.shape, jnp.int32),
            pltpu.VMEM((8, slots), jnp.int32),
            pltpu.VMEM((n_res, 128), jnp.int32),
            pltpu.SMEM((8, slots), jnp.int32),
            pltpu.SMEM((n_res, 128), jnp.int32),
            pltpu.VMEM((amplitudes.shape[0] + 1, tile, tile), bf16),
            pltpu.VMEM(integrals.shape, bf16),
            pltpu.VMEM((n_group * fetch_cap, tile, tile), bf16),
            pltpu.VMEM((n_group - 1, fetch_cap, tile, tile), bf16),
            pltpu.SMEM((n_group - 1,) + requests.shape, jnp.int32),
            pltpu.VMEM((n_blocks, tile, tile), f32),
            pltpu.VMEM((n_z, tile, tile), f32),
            pltpu.VMEM((n_z, tile, tile), f32),
            pltpu.VMEM((n_z - 1, tile, tile), f32),
            pltpu.VMEM((n_z - 1, tile, tile), f32),
            dma((7,)),
            dma((n_group - 1,)),
            dma((n_group - 1,)),
            dma((n_group - 1,)),
            dma((n_group - 1,)),
            dma,
            dma,
            dma((n_z - 1,)),
            dma((n_z - 1,)),
        ],
        compiler_params=pltpu.CompilerParams(
            collective_id=0, has_side_effects=True, vmem_limit_bytes=67043328
        ),
    )(requests, tasks.T, counts, amplitudes, integrals)


SUB = 8
CODES = 32767.0


def count_weights(n_bins, n_res, n_amps, parts, count, task_ref, e_ref, row_ref):
    cap = task_ref.shape[1]
    width = parts * n_amps * SUB
    share = -(-cap // parts)
    bins = task_ref[1:2, :] * n_res + task_ref[2:3, :]
    lane = lax.broadcasted_iota(jnp.int32, (1, cap), 1)
    amp = task_ref[0:1, :]
    for p in range(1, parts):
        amp = amp + jnp.where(lane >= p * share, n_amps, 0)
    hit_bin = (lax.broadcasted_iota(jnp.int32, (n_bins, cap), 0) == bins) & (
        lax.broadcasted_iota(jnp.int32, (n_bins, cap), 1) < count
    )
    first = amp * SUB
    rows = lax.broadcasted_iota(jnp.int32, (width, cap), 0)
    hit_amp = (rows >= first) & (rows < first + SUB)
    row_ref[...] = lax.dot_general(
        jnp.where(hit_bin, 1.0, 0.0).astype(jnp.bfloat16),
        jnp.where(hit_amp, 1.0, 0.0).astype(jnp.bfloat16),
        (((1,), (1,)), ((), ())),
        preferred_element_type=jnp.float32,
    )
    same = jnp.where(
        lax.broadcasted_iota(jnp.int32, (SUB, width), 1) % SUB
        == lax.broadcasted_iota(jnp.int32, (SUB, width), 0),
        1.0, 0.0,
    )
    for b in range(0, n_bins, 2):
        pair = [jnp.broadcast_to(row_ref[b + t:b + t + 1, :], (SUB, width)) * same for t in range(2)]
        e_ref[b * SUB:(b + 2) * SUB, :] = jnp.concatenate(pair, axis=0).astype(jnp.bfloat16)


def combine_amps(n_group, n_res, fetch_cap, parts, amps, e_ref, hi_ref, lo_ref):
    n_amps, tile = amps.shape[0], amps.shape[1]
    block = fetch_cap * n_res * SUB

    def rows16(q, carry):
        base = pl.multiple_of(q * 2 * SUB, 2 * SUB)
        rows = amps[:, pl.ds(base, 2 * SUB), :].astype(jnp.float32)
        halves = [
            rows[:, t * SUB:(t + 1) * SUB, :].reshape(n_amps * SUB, tile).astype(jnp.bfloat16) for t in range(2)
        ]
        right = jnp.concatenate(halves, axis=1)
        right = jnp.concatenate([right] * parts, axis=0)
        for h in range(n_group):
            made = jnp.dot(e_ref[h * block:(h + 1) * block, :], right, preferred_element_type=jnp.float32)
            for c in range(fetch_cap):
                for r in range(n_res):
                    at = (c * n_res + r) * SUB
                    value = jnp.concatenate(
                        [made[at:at + SUB, :tile], made[at:at + SUB, tile:]], axis=0
                    )
                    high = value.astype(jnp.bfloat16)
                    low = (value - high.astype(jnp.float32)).astype(jnp.bfloat16)
                    place = (h, pl.ds(pl.multiple_of(r * tile + base, 2 * SUB), 2 * SUB), pl.ds(c * tile, tile))
                    hi_ref[place] = high
                    lo_ref[place] = low
        return carry

    lax.fori_loop(0, tile // (2 * SUB), rows16, 0)


def dense_kernel(
    n_group, n_member, parts,
    request_hbm, task_hbm, count_hbm, amp_hbm, int_hbm, out_ref,
    request_ref, task_ref, count_ref, amps, ints, fetched, outgoing, wanted, row_ref, e_ref, hi_ref, lo_ref, acc,
    half, half_in, code, code_in, scale, scale_in,
    local_sem, far_sem, chain_sem, req_send, req_recv, tile_send, tile_recv, half_send, half_recv,
    code_send, code_recv, scale_send, scale_recv,
):
    g = lax.axis_index("group")
    m = lax.axis_index("member")
    n_z = n_member // 2
    n_res = n_member * RES_DEV
    z, core = m // 2, m % 2
    fetch_cap = request_ref.shape[1]
    tile = amps.shape[1]
    amp_copy = pltpu.make_async_copy(amp_hbm, amps, local_sem.at[0])
    int_copy = pltpu.make_async_copy(int_hbm, ints, local_sem.at[1])
    request_copy = pltpu.make_async_copy(request_hbm, request_ref, local_sem.at[2])
    task_copy = pltpu.make_async_copy(task_hbm, task_ref, local_sem.at[3])
    count_copy = pltpu.make_async_copy(count_hbm, count_ref, local_sem.at[4])
    for copy in (request_copy, int_copy, task_copy, count_copy, amp_copy):
        copy.start()
    row, col = g // 2, g % 2
    near = [row * 2 + 1 - col, (1 - row) * 2 + col]
    partners = near + [(1 - row) * 2 + 1 - col]
    sibling = (g, z * 2 + 1 - core)

    barrier = pltpu.get_barrier_semaphore()

    def greet(device):
        pl.semaphore_signal(barrier, inc=1, device_id=device, device_id_type=MESH)

    for h in near:
        greet((h, m))
    greet(sibling)

    @pl.when(z > 0)
    def _():
        greet((g, m - 2))

    @pl.when(z < n_z - 1)
    def _():
        greet((g, m + 2))

    request_copy.wait()
    ends = jnp.where(z > 0, 1, 0) + jnp.where(z < n_z - 1, 1, 0)
    pl.semaphore_wait(barrier, 3 + ends)

    def ask(i):
        return pltpu.make_async_remote_copy(
            src_ref=request_ref, dst_ref=wanted.at[i], send_sem=req_send.at[i], recv_sem=req_recv.at[i],
            device_id=(partners[i], m), device_id_type=MESH,
        )

    def tiles(i):
        return pltpu.make_async_remote_copy(
            src_ref=outgoing.at[i], dst_ref=fetched.at[i + 1], send_sem=tile_send.at[i], recv_sem=tile_recv.at[i],
            device_id=(partners[i], m), device_id_type=MESH,
        )

    ask(0).start()
    ask(1).start()
    pl.semaphore_signal(far_sem, inc=1, device_id=(near[0], m), device_id_type=MESH)
    up, down = chain_sem.at[0], chain_sem.at[1]

    def tell_up():
        pl.semaphore_signal(up, inc=1, device_id=(g, m + 2), device_id_type=MESH)

    def tell_down():
        pl.semaphore_signal(down, inc=1, device_id=(g, m - 2), device_id_type=MESH)

    @pl.when((z == 1) & (z < n_z - 1))
    def _():
        tell_up()

    @pl.when((z == n_z - 2) & (z > 0))
    def _():
        tell_down()

    count_copy.wait()
    task_copy.wait()
    n_bins = n_group * fetch_cap * n_res
    pl.semaphore_wait(far_sem, 1)
    ask(2).start()
    count_weights(n_bins, n_res, amp_hbm.shape[0], parts, count_ref[0], task_ref, e_ref, row_ref)
    int_copy.wait()
    for c in range(fetch_cap):
        fetched[0, c] = ints[request_ref[g, c]]
    for i in range(n_group - 1):
        ask(i).wait_recv()
        for c in range(fetch_cap):
            outgoing[i, c] = ints[wanted[i, g, c]]
        tiles(i).start()

    @pl.when(z > 1)
    def _():
        pl.semaphore_wait(up, 1)

    @pl.when((z > 1) & (z < n_z - 1))
    def _():
        tell_up()

    @pl.when(z < n_z - 2)
    def _():
        pl.semaphore_wait(down, 1)

    @pl.when((z < n_z - 2) & (z > 0))
    def _():
        tell_down()

    amp_copy.wait()
    combine_amps(n_group, n_res, fetch_cap, parts, amps, e_ref, hi_ref, lo_ref)

    def product(i, r):
        h = g if i == 0 else partners[i - 1]
        rows = pl.ds(pl.multiple_of(r * tile, tile), tile)
        right = fetched[i].reshape(fetch_cap * tile, tile)
        return jnp.dot(hi_ref[h, rows, :], right, preferred_element_type=jnp.float32) + jnp.dot(
            lo_ref[h, rows, :], right, preferred_element_type=jnp.float32
        )

    for i in range(n_group - 1):
        if i > 0:
            tiles(i - 1).wait_recv()

        def add(r, carry, i=i):
            value = product(i, r)
            acc[r] = value if i == 0 else acc[r] + value
            return carry

        lax.fori_loop(0, n_res, add, 0)
    last = n_group - 1
    tiles(last - 1).wait_recv()

    low_end = z < n_z // 2

    def order(t):
        down_v = n_z - 1 - t
        down_k = jnp.where(down_v > z, down_v, down_v - 1)
        up_k = jnp.where(t < z, t, t + 1)
        return jnp.where(low_end, down_k, up_k)

    def swap(k):
        return pltpu.make_async_remote_copy(
            src_ref=half.at[k], dst_ref=half_in.at[k], send_sem=half_send.at[k], recv_sem=half_recv.at[k],
            device_id=sibling, device_id_type=MESH,
        )

    ks = [order(t) for t in range(n_z - 1)] + [z]
    for k in ks:
        r = 2 * k + 1 - core
        half[k] = acc[r] + product(last, r)
        swap(k).start()
    for k in ks:
        r = 2 * k + core
        acc[r] = acc[r] + product(last, r)

    def sends(k):
        return [
            pltpu.make_async_remote_copy(
                src_ref=s.at[k], dst_ref=d.at[z], send_sem=ss.at[k], recv_sem=rs.at[z],
                device_id=(g, 2 * k + core), device_id_type=MESH,
            )
            for s, d, ss, rs in (
                (scale, scale_in, scale_send, scale_recv), (code, code_in, code_send, code_recv),
            )
        ]

    def arrivals(k):
        return [
            pltpu.make_async_remote_copy(
                src_ref=s.at[k], dst_ref=d.at[k], send_sem=ss.at[k], recv_sem=rs.at[k],
                device_id=(g, 2 * k + core), device_id_type=MESH,
            )
            for s, d, ss, rs in (
                (scale, scale_in, scale_send, scale_recv), (code, code_in, code_send, code_recv),
            )
        ]

    for k in ks[:-1]:
        swap(k).wait_recv()
        value = acc[2 * k + core] + half_in[k]
        top = jnp.maximum(jnp.max(jnp.abs(value), axis=0, keepdims=True), 1e-30)
        scale[k] = jnp.broadcast_to(top * (1.0 / CODES), (SUB, tile))
        code[k] = jnp.round(value * (CODES / top)).astype(jnp.int32).astype(jnp.int16)
        for copy in sends(k):
            copy.start()
    swap(z).wait_recv()
    result = acc[m] + half_in[z]
    for k in reversed(ks[:-1]):
        for copy in arrivals(k):
            copy.wait_recv()
        part = code_in[k].astype(jnp.int32).astype(jnp.float32)
        result = result + part * scale_in[k][:1, :]
    out_ref[0] = result
    for i in range(n_group - 1):
        ask(i).wait_send()
        tiles(i).wait_send()
    for k in ks:
        swap(k).wait_send()
    for k in ks[:-1]:
        for copy in sends(k):
            copy.wait_send()


def dense_call(amplitudes, integrals, tasks, requests, counts):
    n_amps, tile = amplitudes.shape[0], amplitudes.shape[1]
    n_group = lax.axis_size("group")
    n_member = lax.axis_size("member")
    n_res = RES_DEV * n_member
    n_z = n_member // 2
    cap = tasks.shape[0]
    fetch_cap = requests.shape[1]
    n_bins = n_group * fetch_cap * n_res
    parts = -(-cap // 256)
    width = parts * n_amps * SUB
    vmem = pl.BlockSpec(memory_space=pltpu.VMEM)
    hbm = pl.BlockSpec(memory_space=pltpu.HBM)
    f32, bf16 = jnp.float32, amplitudes.dtype
    dma = pltpu.SemaphoreType.DMA
    return pl.pallas_call(
        functools.partial(dense_kernel, n_group, n_member, parts),
        out_shape=jax.ShapeDtypeStruct((RES_DEV, tile, tile), f32),
        in_specs=[hbm] * 5,
        out_specs=vmem,
        scratch_shapes=[
            pltpu.SMEM(requests.shape, jnp.int32),
            pltpu.VMEM((tasks.shape[1], cap), jnp.int32),
            pltpu.SMEM(counts.shape, jnp.int32),
            pltpu.VMEM(amplitudes.shape, bf16),
            pltpu.VMEM(integrals.shape, bf16),
            pltpu.VMEM((n_group, fetch_cap, tile, tile), bf16),
            pltpu.VMEM((n_group - 1, fetch_cap, tile, tile), bf16),
            pltpu.SMEM((n_group - 1,) + requests.shape, jnp.int32),
            pltpu.VMEM((n_bins, width), f32),
            pltpu.VMEM((n_bins * SUB, width), bf16),
            pltpu.VMEM((n_group, n_res * tile, fetch_cap * tile), bf16),
            pltpu.VMEM((n_group, n_res * tile, fetch_cap * tile), bf16),
            pltpu.VMEM((n_res, tile, tile), f32),
            pltpu.VMEM((n_z, tile, tile), f32),
            pltpu.VMEM((n_z, tile, tile), f32),
            pltpu.VMEM((n_z, tile, tile), jnp.int16),
            pltpu.VMEM((n_z, tile, tile), jnp.int16),
            pltpu.VMEM((n_z, SUB, tile), f32),
            pltpu.VMEM((n_z, SUB, tile), f32),
            dma((5,)),
            pltpu.SemaphoreType.REGULAR,
            pltpu.SemaphoreType.REGULAR((2,)),
            dma((n_group - 1,)),
            dma((n_group - 1,)),
            dma((n_group - 1,)),
            dma((n_group - 1,)),
            dma((n_z,)),
            dma((n_z,)),
            dma((n_z,)),
            dma((n_z,)),
            dma((n_z,)),
            dma((n_z,)),
        ],
        compiler_params=pltpu.CompilerParams(
            collective_id=0, has_side_effects=True, vmem_limit_bytes=50331648
        ),
    )(requests, tasks.T, counts, amplitudes, integrals)


def per_device(amplitudes, integrals, tasks, requests, counts):
    n_bins = lax.axis_size("group") * requests.shape[1] * lax.axis_size("member") * RES_DEV
    if lax.axis_size("group") == 4 and n_bins * 2 <= tasks.shape[0]:
        return dense_call(amplitudes, integrals, tasks, requests, counts)
    return sorted_tasks_call(amplitudes, integrals, tasks, requests, counts)


def solution(mesh):
    return jax.shard_map(
        per_device,
        mesh=mesh,
        in_specs=(
            P(("group", "member"), None, None),
            P(("group", "member"), None, None),
            P(("group", "member"), None),
            P(("group", "member"), None),
            P(("group", "member")),
        ),
        out_specs=P(("group", "member"), None, None),
        check_vma=False,
    )
```

```python
import functools

import jax
import jax.numpy as jnp
from jax import lax
from jax.experimental import pallas as pl
from jax.experimental.pallas import tpu as pltpu
from jax.sharding import PartitionSpec as P

RES_DEV = 1
BLOCK = 8
UNROLL = 8
MESH = pl.DeviceIdType.MESH


def round_up(n, k):
    return (n + k - 1) // k * k


def sort_tasks(n_res, n_blocks, n_amps, n_fetched, count, task_ref, slot_ref, last_ref):
    cap = task_ref.shape[1]
    slots = slot_ref.shape[1]
    valid = lax.broadcasted_iota(jnp.int32, (n_res, cap), 1) < count
    rows = lax.broadcasted_iota(jnp.int32, (n_res, cap), 0)
    hit = jnp.where(valid & (rows == task_ref[2:3, :]), 1.0, 0.0)
    upper = jnp.where(
        lax.broadcasted_iota(jnp.int32, (cap, cap), 0) <= lax.broadcasted_iota(jnp.int32, (cap, cap), 1), 1.0, 0.0
    ).astype(jnp.bfloat16)
    rank = jnp.dot(hit.astype(jnp.bfloat16), upper, preferred_element_type=jnp.float32)
    number = jnp.sum(hit, axis=1, keepdims=True).astype(jnp.int32)
    blocks = jnp.maximum((number + (BLOCK - 1)) // BLOCK, 1)
    blocks = jnp.broadcast_to(blocks, (n_res, 128))
    lower = jnp.where(
        lax.broadcasted_iota(jnp.int32, (n_res, n_res), 1) < lax.broadcasted_iota(jnp.int32, (n_res, n_res), 0), 1.0, 0.0
    ).astype(jnp.bfloat16)
    first = jnp.dot(
        lower, blocks.astype(jnp.float32).astype(jnp.bfloat16), preferred_element_type=jnp.float32
    ).astype(jnp.int32)
    last_ref[...] = jnp.clip(first + blocks - 1, 0, n_blocks - 1)
    place = jnp.sum(hit * (rank + (first[:, :1] * BLOCK).astype(jnp.float32)), axis=0, keepdims=True) - 1.0
    place = place.astype(jnp.int32)
    chosen = jnp.where(lax.broadcasted_iota(jnp.int32, (slots, cap), 0) == place, 1.0, 0.0).astype(jnp.bfloat16)
    line = lax.broadcasted_iota(jnp.int32, (8, cap), 0)
    values = jnp.where(line == 0, task_ref[0:1, :] + 1, jnp.where(line == 1, task_ref[1:2, :], 0))
    picked = lax.dot_general(
        values.astype(jnp.float32).astype(jnp.bfloat16),
        chosen,
        (((1,), (1,)), ((), ())),
        preferred_element_type=jnp.float32,
    ).astype(jnp.int32)
    starts = jnp.sum(jnp.where(lax.broadcasted_iota(jnp.int32, (n_res, 128), 1) == first, 1, 0), axis=0, keepdims=True)
    keep = jnp.concatenate([1 - starts, jnp.zeros((1, slots - 128), jnp.int32)], axis=1)
    picked = jnp.clip(picked, 0, jnp.where(lax.broadcasted_iota(jnp.int32, (8, slots), 0) == 0, n_amps, n_fetched - 1))
    slot_ref[...] = jnp.where(lax.broadcasted_iota(jnp.int32, (8, slots), 0) == 2, keep, picked)


def main_kernel(
    n_group, n_member, n_blocks,
    request_hbm, task_hbm, count_hbm, amp_hbm, int_hbm, out_ref,
    request_ref, task_ref, count_ref, slot_vmem, last_vmem, slot_ref, last_ref, amps, ints, fetched, outgoing, wanted, running, half, half_in, pair, pair_in,
    local_sem, req_send, req_recv, tile_send, tile_recv, half_send, half_recv, pair_send, pair_recv,
):
    g = lax.axis_index("group")
    m = lax.axis_index("member")
    n_z = n_member // 2
    z, core = m // 2, m % 2
    fetch_cap = request_ref.shape[1]
    tile = amps.shape[1]
    amp_copy = pltpu.make_async_copy(amp_hbm, amps.at[pl.ds(1, amp_hbm.shape[0])], local_sem.at[0])
    int_copy = pltpu.make_async_copy(int_hbm, ints, local_sem.at[1])
    request_copy = pltpu.make_async_copy(request_hbm, request_ref, local_sem.at[2])
    task_copy = pltpu.make_async_copy(task_hbm, task_ref, local_sem.at[3])
    count_copy = pltpu.make_async_copy(count_hbm, count_ref, local_sem.at[4])
    for copy in (request_copy, int_copy, task_copy, count_copy, amp_copy):
        copy.start()
    group_peers = [((g + i) % n_group, m) for i in range(1, n_group)]
    sibling = (g, z * 2 + 1 - core)
    z_peers = [(g, ((z + i) % n_z) * 2 + core) for i in range(1, n_z)]

    barrier = pltpu.get_barrier_semaphore()
    for peer in group_peers + [sibling] + z_peers:
        pl.semaphore_signal(barrier, inc=1, device_id=peer, device_id_type=MESH)
    amps[0] = jnp.zeros((tile, tile), amps.dtype)
    request_copy.wait()
    pl.semaphore_wait(barrier, n_group + n_z - 1)

    asks = []
    for i, peer in enumerate(group_peers):
        ask = pltpu.make_async_remote_copy(
            src_ref=request_ref, dst_ref=wanted.at[i], send_sem=req_send.at[i], recv_sem=req_recv.at[i],
            device_id=peer, device_id_type=MESH,
        )
        ask.start()
        asks.append(ask)
    int_copy.wait()
    for c in range(fetch_cap):
        fetched[g * fetch_cap + c] = ints[request_ref[g, c]]
    sends = []
    for i in range(n_group - 1):
        asks[i].wait_recv()
        for c in range(fetch_cap):
            outgoing[i, c] = ints[wanted[i, g, c]]
        send = pltpu.make_async_remote_copy(
            src_ref=outgoing.at[i], dst_ref=fetched.at[pl.ds(g * fetch_cap, fetch_cap)],
            send_sem=tile_send.at[i], recv_sem=tile_recv.at[i],
            device_id=((g + n_group - i - 1) % n_group, m), device_id_type=MESH,
        )
        send.start()
        sends.append(send)
    count_copy.wait()
    task_copy.wait()
    sort_tasks(
        n_member * RES_DEV, n_blocks, amp_hbm.shape[0], fetched.shape[0], count_ref[0], task_ref, slot_vmem, last_vmem,
    )
    slot_copy = pltpu.make_async_copy(slot_vmem, slot_ref, local_sem.at[5])
    last_copy = pltpu.make_async_copy(last_vmem, last_ref, local_sem.at[6])
    slot_copy.start()
    last_copy.start()
    amp_copy.wait()
    slot_copy.wait()
    last_copy.wait()
    for i in range(n_group - 1):
        asks[i].wait_send()
        source = (g + i + 1) % n_group
        pltpu.make_async_remote_copy(
            src_ref=outgoing.at[i], dst_ref=fetched.at[pl.ds(source * fetch_cap, fetch_cap)],
            send_sem=tile_send.at[i], recv_sem=tile_recv.at[i],
            device_id=group_peers[i], device_id_type=MESH,
        ).wait_recv()

    def block(b, total):
        for u in range(UNROLL):
            total = one_block(b * UNROLL + u, total)
        return total

    def one_block(b, total):
        left = []
        right = []
        for t in range(BLOCK):
            left.append(amps[slot_ref[0, b * BLOCK + t]])
            right.append(fetched[slot_ref[1, b * BLOCK + t]])
        product = jnp.dot(
            jnp.concatenate(left, axis=1), jnp.concatenate(right, axis=0), preferred_element_type=jnp.float32
        )
        total = jnp.where(slot_ref[2, b] != 0, total, 0.0) + product
        running[b] = total
        return total

    lax.fori_loop(0, n_blocks // UNROLL, block, jnp.zeros((tile, tile), jnp.float32))

    for k in range(n_z):
        half[k] = running[last_ref[2 * k + 1 - core, 0]]
    swap = pltpu.make_async_remote_copy(
        src_ref=half, dst_ref=half_in, send_sem=half_send, recv_sem=half_recv,
        device_id=sibling, device_id_type=MESH,
    )
    swap.start()
    swap.wait_recv()
    parts = []
    for i in range(1, n_z):
        k = (z + i) % n_z
        pair[i - 1] = running[last_ref[2 * k + core, 0]] + half_in[k]
        part = pltpu.make_async_remote_copy(
            src_ref=pair.at[i - 1], dst_ref=pair_in.at[i - 1],
            send_sem=pair_send.at[i - 1], recv_sem=pair_recv.at[i - 1],
            device_id=z_peers[i - 1], device_id_type=MESH,
        )
        part.start()
        parts.append(part)
    result = running[last_ref[m, 0]] + half_in[z]
    for i in range(n_z - 1):
        parts[i].wait_recv()
        result = result + pair_in[i]
    out_ref[0] = result
    swap.wait_send()
    for copy in sends + parts:
        copy.wait_send()


def sorted_tasks_call(amplitudes, integrals, tasks, requests, counts):
    tile = amplitudes.shape[1]
    n_group = lax.axis_size("group")
    n_member = lax.axis_size("member")
    n_res = RES_DEV * n_member
    cap = tasks.shape[0]
    fetch_cap = requests.shape[1]
    n_z = n_member // 2
    n_blocks = round_up((cap + BLOCK - 1) // BLOCK + n_res, UNROLL)
    slots = round_up(n_blocks * BLOCK, 128)
    vmem = pl.BlockSpec(memory_space=pltpu.VMEM)
    hbm = pl.BlockSpec(memory_space=pltpu.HBM)
    f32, bf16 = jnp.float32, amplitudes.dtype
    dma = pltpu.SemaphoreType.DMA
    return pl.pallas_call(
        functools.partial(main_kernel, n_group, n_member, n_blocks),
        out_shape=jax.ShapeDtypeStruct((RES_DEV, tile, tile), f32),
        in_specs=[hbm] * 5,
        out_specs=vmem,
        scratch_shapes=[
            pltpu.SMEM(requests.shape, jnp.int32),
            pltpu.VMEM((tasks.shape[1], cap), jnp.int32),
            pltpu.SMEM(counts.shape, jnp.int32),
            pltpu.VMEM((8, slots), jnp.int32),
            pltpu.VMEM((n_res, 128), jnp.int32),
            pltpu.SMEM((8, slots), jnp.int32),
            pltpu.SMEM((n_res, 128), jnp.int32),
            pltpu.VMEM((amplitudes.shape[0] + 1, tile, tile), bf16),
            pltpu.VMEM(integrals.shape, bf16),
            pltpu.VMEM((n_group * fetch_cap, tile, tile), bf16),
            pltpu.VMEM((n_group - 1, fetch_cap, tile, tile), bf16),
            pltpu.SMEM((n_group - 1,) + requests.shape, jnp.int32),
            pltpu.VMEM((n_blocks, tile, tile), f32),
            pltpu.VMEM((n_z, tile, tile), f32),
            pltpu.VMEM((n_z, tile, tile), f32),
            pltpu.VMEM((n_z - 1, tile, tile), f32),
            pltpu.VMEM((n_z - 1, tile, tile), f32),
            dma((7,)),
            dma((n_group - 1,)),
            dma((n_group - 1,)),
            dma((n_group - 1,)),
            dma((n_group - 1,)),
            dma,
            dma,
            dma((n_z - 1,)),
            dma((n_z - 1,)),
        ],
        compiler_params=pltpu.CompilerParams(
            collective_id=0, has_side_effects=True, vmem_limit_bytes=67043328
        ),
    )(requests, tasks.T, counts, amplitudes, integrals)


SUB = 8
CODES = 32767.0


def count_weights(n_bins, n_res, n_amps, parts, count, task_ref, e_ref, row_ref):
    cap = task_ref.shape[1]
    width = parts * n_amps * SUB
    share = -(-cap // parts)
    bins = task_ref[1:2, :] * n_res + task_ref[2:3, :]
    lane = lax.broadcasted_iota(jnp.int32, (1, cap), 1)
    amp = task_ref[0:1, :]
    for p in range(1, parts):
        amp = amp + jnp.where(lane >= p * share, n_amps, 0)
    hit_bin = (lax.broadcasted_iota(jnp.int32, (n_bins, cap), 0) == bins) & (
        lax.broadcasted_iota(jnp.int32, (n_bins, cap), 1) < count
    )
    first = amp * SUB
    rows = lax.broadcasted_iota(jnp.int32, (width, cap), 0)
    hit_amp = (rows >= first) & (rows < first + SUB)
    row_ref[...] = lax.dot_general(
        jnp.where(hit_bin, 1.0, 0.0).astype(jnp.bfloat16),
        jnp.where(hit_amp, 1.0, 0.0).astype(jnp.bfloat16),
        (((1,), (1,)), ((), ())),
        preferred_element_type=jnp.float32,
    )
    same = jnp.where(
        lax.broadcasted_iota(jnp.int32, (SUB, width), 1) % SUB
        == lax.broadcasted_iota(jnp.int32, (SUB, width), 0),
        1.0, 0.0,
    )
    for b in range(0, n_bins, 2):
        pair = [jnp.broadcast_to(row_ref[b + t:b + t + 1, :], (SUB, width)) * same for t in range(2)]
        e_ref[b * SUB:(b + 2) * SUB, :] = jnp.concatenate(pair, axis=0).astype(jnp.bfloat16)


def combine_amps(n_group, n_res, fetch_cap, parts, amps, e_ref, hi_ref, lo_ref):
    n_amps, tile = amps.shape[0], amps.shape[1]
    block = fetch_cap * n_res * SUB

    def rows16(q, carry):
        base = pl.multiple_of(q * 2 * SUB, 2 * SUB)
        rows = amps[:, pl.ds(base, 2 * SUB), :].astype(jnp.float32)
        halves = [
            rows[:, t * SUB:(t + 1) * SUB, :].reshape(n_amps * SUB, tile).astype(jnp.bfloat16) for t in range(2)
        ]
        right = jnp.concatenate(halves, axis=1)
        right = jnp.concatenate([right] * parts, axis=0)
        for h in range(n_group):
            made = jnp.dot(e_ref[h * block:(h + 1) * block, :], right, preferred_element_type=jnp.float32)
            for c in range(fetch_cap):
                for r in range(n_res):
                    at = (c * n_res + r) * SUB
                    value = jnp.concatenate(
                        [made[at:at + SUB, :tile], made[at:at + SUB, tile:]], axis=0
                    )
                    high = value.astype(jnp.bfloat16)
                    low = (value - high.astype(jnp.float32)).astype(jnp.bfloat16)
                    place = (h, pl.ds(pl.multiple_of(r * tile + base, 2 * SUB), 2 * SUB), pl.ds(c * tile, tile))
                    hi_ref[place] = high
                    lo_ref[place] = low
        return carry

    lax.fori_loop(0, tile // (2 * SUB), rows16, 0)


def dense_kernel(
    n_group, n_member, parts,
    request_hbm, task_hbm, count_ref, amp_hbm, int_hbm, out_ref,
    request_ref, task_ref, amps, ints, fetched, outgoing, wanted, row_ref, e_ref, hi_ref, lo_ref, acc,
    half, half_in, code, code_in, scale, scale_in,
    local_sem, far_sem, chain_sem, req_send, req_recv, tile_send, tile_recv, half_send, half_recv,
    code_send, code_recv, scale_send, scale_recv,
):
    g = lax.axis_index("group")
    m = lax.axis_index("member")
    n_z = n_member // 2
    n_res = n_member * RES_DEV
    z, core = m // 2, m % 2
    fetch_cap = request_ref.shape[1]
    tile = amps.shape[1]
    amp_copy = pltpu.make_async_copy(amp_hbm, amps, local_sem.at[0])
    int_copy = pltpu.make_async_copy(int_hbm, ints, local_sem.at[1])
    request_copy = pltpu.make_async_copy(request_hbm, request_ref, local_sem.at[2])
    task_copy = pltpu.make_async_copy(task_hbm, task_ref, local_sem.at[3])
    for copy in (request_copy, int_copy, task_copy, amp_copy):
        copy.start()
    row, col = g // 2, g % 2
    near = [row * 2 + 1 - col, (1 - row) * 2 + col]
    partners = near + [(1 - row) * 2 + 1 - col]
    sibling = (g, z * 2 + 1 - core)

    barrier = pltpu.get_barrier_semaphore()

    def greet(device):
        pl.semaphore_signal(barrier, inc=1, device_id=device, device_id_type=MESH)

    for h in near:
        greet((h, m))
    greet(sibling)

    @pl.when(z > 0)
    def _():
        greet((g, m - 2))

    @pl.when(z < n_z - 1)
    def _():
        greet((g, m + 2))

    request_copy.wait()
    ends = jnp.where(z > 0, 1, 0) + jnp.where(z < n_z - 1, 1, 0)
    pl.semaphore_wait(barrier, 3 + ends)

    def ask(i):
        return pltpu.make_async_remote_copy(
            src_ref=request_ref, dst_ref=wanted.at[i], send_sem=req_send.at[i], recv_sem=req_recv.at[i],
            device_id=(partners[i], m), device_id_type=MESH,
        )

    def tiles(i):
        return pltpu.make_async_remote_copy(
            src_ref=outgoing.at[i], dst_ref=fetched.at[i + 1], send_sem=tile_send.at[i], recv_sem=tile_recv.at[i],
            device_id=(partners[i], m), device_id_type=MESH,
        )

    ask(0).start()
    ask(1).start()
    pl.semaphore_signal(far_sem, inc=1, device_id=(near[0], m), device_id_type=MESH)
    up, down = chain_sem.at[0], chain_sem.at[1]

    def tell_up():
        pl.semaphore_signal(up, inc=1, device_id=(g, m + 2), device_id_type=MESH)

    def tell_down():
        pl.semaphore_signal(down, inc=1, device_id=(g, m - 2), device_id_type=MESH)

    @pl.when((z == 1) & (z < n_z - 1))
    def _():
        tell_up()

    @pl.when((z == n_z - 2) & (z > 0))
    def _():
        tell_down()

    task_copy.wait()
    n_bins = n_group * fetch_cap * n_res
    pl.semaphore_wait(far_sem, 1)
    ask(2).start()
    count_weights(n_bins, n_res, amp_hbm.shape[0], parts, count_ref[0], task_ref, e_ref, row_ref)
    int_copy.wait()
    for c in range(fetch_cap):
        fetched[0, c] = ints[request_ref[g, c]]
    for i in range(n_group - 1):
        ask(i).wait_recv()
        for c in range(fetch_cap):
            outgoing[i, c] = ints[wanted[i, g, c]]
        tiles(i).start()

    amp_copy.wait()
    combine_amps(n_group, n_res, fetch_cap, parts, amps, e_ref, hi_ref, lo_ref)

    @pl.when((z > 1) & (z < n_z - 1))
    def _():
        pl.semaphore_wait(up, 1)
        tell_up()

    @pl.when((z < n_z - 2) & (z > 0))
    def _():
        pl.semaphore_wait(down, 1)
        tell_down()

    def product(i, r):
        h = g if i == 0 else partners[i - 1]
        rows = pl.ds(pl.multiple_of(r * tile, tile), tile)
        right = fetched[i].reshape(fetch_cap * tile, tile)
        return jnp.dot(hi_ref[h, rows, :], right, preferred_element_type=jnp.float32) + jnp.dot(
            lo_ref[h, rows, :], right, preferred_element_type=jnp.float32
        )

    for i in range(n_group - 1):
        if i > 0:
            tiles(i - 1).wait_recv()

        for r in range(n_res):
            value = product(i, r)
            acc[r] = value if i == 0 else acc[r] + value
    @pl.when((z > 1) & (z == n_z - 1))
    def _():
        pl.semaphore_wait(up, 1)

    @pl.when((z < n_z - 2) & (z == 0))
    def _():
        pl.semaphore_wait(down, 1)

    last = n_group - 1
    tiles(last - 1).wait_recv()

    low_end = z < n_z // 2

    def order(t):
        down_v = n_z - 1 - t
        down_k = jnp.where(down_v > z, down_v, down_v - 1)
        up_k = jnp.where(t < z, t, t + 1)
        return jnp.where(low_end, down_k, up_k)

    def swap(k):
        return pltpu.make_async_remote_copy(
            src_ref=half.at[k], dst_ref=half_in.at[k], send_sem=half_send.at[k], recv_sem=half_recv.at[k],
            device_id=sibling, device_id_type=MESH,
        )

    ks = [order(t) for t in range(n_z - 1)] + [z]
    for k in ks:
        r = 2 * k + 1 - core
        half[k] = acc[r] + product(last, r)
        swap(k).start()
    for k in ks:
        r = 2 * k + core
        acc[r] = acc[r] + product(last, r)

    def sends(k):
        return [
            pltpu.make_async_remote_copy(
                src_ref=s.at[k], dst_ref=d.at[z], send_sem=ss.at[k], recv_sem=rs.at[z],
                device_id=(g, 2 * k + core), device_id_type=MESH,
            )
            for s, d, ss, rs in (
                (scale, scale_in, scale_send, scale_recv), (code, code_in, code_send, code_recv),
            )
        ]

    def arrivals(k):
        return [
            pltpu.make_async_remote_copy(
                src_ref=s.at[k], dst_ref=d.at[k], send_sem=ss.at[k], recv_sem=rs.at[k],
                device_id=(g, 2 * k + core), device_id_type=MESH,
            )
            for s, d, ss, rs in (
                (scale, scale_in, scale_send, scale_recv), (code, code_in, code_send, code_recv),
            )
        ]

    for k in ks[:-1]:
        swap(k).wait_recv()
        value = acc[2 * k + core] + half_in[k]
        top = jnp.maximum(jnp.max(jnp.abs(value), axis=0, keepdims=True), 1e-30)
        scale[k] = jnp.broadcast_to(top * (1.0 / CODES), (SUB, tile))
        code[k] = jnp.round(value * (CODES / top)).astype(jnp.int32).astype(jnp.int16)
        for copy in sends(k):
            copy.start()
    swap(z).wait_recv()
    result = acc[m] + half_in[z]
    for k in reversed(ks[:-1]):
        for copy in arrivals(k):
            copy.wait_recv()
        part = code_in[k].astype(jnp.int32).astype(jnp.float32)
        result = result + part * scale_in[k][:1, :]
    out_ref[0] = result
    for i in range(n_group - 1):
        ask(i).wait_send()
        tiles(i).wait_send()
    for k in ks:
        swap(k).wait_send()
    for k in ks[:-1]:
        for copy in sends(k):
            copy.wait_send()


def dense_call(amplitudes, integrals, tasks, requests, counts):
    n_amps, tile = amplitudes.shape[0], amplitudes.shape[1]
    pin = functools.partial(pltpu.with_memory_space_constraint, memory_space=pltpu.HBM)
    n_group = lax.axis_size("group")
    n_member = lax.axis_size("member")
    n_res = RES_DEV * n_member
    n_z = n_member // 2
    cap = tasks.shape[0]
    fetch_cap = requests.shape[1]
    n_bins = n_group * fetch_cap * n_res
    parts = -(-cap // 256)
    width = parts * n_amps * SUB
    vmem = pl.BlockSpec(memory_space=pltpu.VMEM)
    hbm = pl.BlockSpec(memory_space=pltpu.HBM)
    f32, bf16 = jnp.float32, amplitudes.dtype
    dma = pltpu.SemaphoreType.DMA
    return pl.pallas_call(
        functools.partial(dense_kernel, n_group, n_member, parts),
        out_shape=jax.ShapeDtypeStruct((RES_DEV, tile, tile), f32),
        in_specs=[hbm, hbm, pl.BlockSpec(memory_space=pltpu.SMEM), hbm, hbm],
        out_specs=vmem,
        scratch_shapes=[
            pltpu.SMEM(requests.shape, jnp.int32),
            pltpu.VMEM((tasks.shape[1], cap), jnp.int32),
            pltpu.VMEM(amplitudes.shape, bf16),
            pltpu.VMEM(integrals.shape, bf16),
            pltpu.VMEM((n_group, fetch_cap, tile, tile), bf16),
            pltpu.VMEM((n_group - 1, fetch_cap, tile, tile), bf16),
            pltpu.SMEM((n_group - 1,) + requests.shape, jnp.int32),
            pltpu.VMEM((n_bins, width), f32),
            pltpu.VMEM((n_bins * SUB, width), bf16),
            pltpu.VMEM((n_group, n_res * tile, fetch_cap * tile), bf16),
            pltpu.VMEM((n_group, n_res * tile, fetch_cap * tile), bf16),
            pltpu.VMEM((n_res, tile, tile), f32),
            pltpu.VMEM((n_z, tile, tile), f32),
            pltpu.VMEM((n_z, tile, tile), f32),
            pltpu.VMEM((n_z, tile, tile), jnp.int16),
            pltpu.VMEM((n_z, tile, tile), jnp.int16),
            pltpu.VMEM((n_z, SUB, tile), f32),
            pltpu.VMEM((n_z, SUB, tile), f32),
            dma((5,)),
            pltpu.SemaphoreType.REGULAR,
            pltpu.SemaphoreType.REGULAR((2,)),
            dma((n_group - 1,)),
            dma((n_group - 1,)),
            dma((n_group - 1,)),
            dma((n_group - 1,)),
            dma((n_z,)),
            dma((n_z,)),
            dma((n_z,)),
            dma((n_z,)),
            dma((n_z,)),
            dma((n_z,)),
        ],
        compiler_params=pltpu.CompilerParams(
            collective_id=0, has_side_effects=True, vmem_limit_bytes=50331648
        ),
    )(pin(requests), pin(tasks.T), counts, pin(amplitudes), pin(integrals))


def per_device(amplitudes, integrals, tasks, requests, counts):
    n_bins = lax.axis_size("group") * requests.shape[1] * lax.axis_size("member") * RES_DEV
    if lax.axis_size("group") == 4 and n_bins * 2 <= tasks.shape[0]:
        return dense_call(amplitudes, integrals, tasks, requests, counts)
    return sorted_tasks_call(amplitudes, integrals, tasks, requests, counts)


def solution(mesh):
    return jax.shard_map(
        per_device,
        mesh=mesh,
        in_specs=(
            P(("group", "member"), None, None),
            P(("group", "member"), None, None),
            P(("group", "member"), None),
            P(("group", "member"), None),
            P(("group", "member")),
        ),
        out_specs=P(("group", "member"), None, None),
        check_vma=False,
    )
```

```python
import functools

import jax
import jax.numpy as jnp
from jax import lax
from jax.experimental import pallas as pl
from jax.experimental.pallas import tpu as pltpu
from jax.sharding import PartitionSpec as P

RES_DEV = 1
BLOCK = 8
UNROLL = 8
MESH = pl.DeviceIdType.MESH


def round_up(n, k):
    return (n + k - 1) // k * k


def sort_tasks(n_res, n_blocks, n_amps, n_fetched, count, task_ref, slot_ref, last_ref):
    cap = task_ref.shape[1]
    slots = slot_ref.shape[1]
    valid = lax.broadcasted_iota(jnp.int32, (n_res, cap), 1) < count
    rows = lax.broadcasted_iota(jnp.int32, (n_res, cap), 0)
    hit = jnp.where(valid & (rows == task_ref[2:3, :]), 1.0, 0.0)
    upper = jnp.where(
        lax.broadcasted_iota(jnp.int32, (cap, cap), 0) <= lax.broadcasted_iota(jnp.int32, (cap, cap), 1), 1.0, 0.0
    ).astype(jnp.bfloat16)
    rank = jnp.dot(hit.astype(jnp.bfloat16), upper, preferred_element_type=jnp.float32)
    number = jnp.sum(hit, axis=1, keepdims=True).astype(jnp.int32)
    blocks = jnp.maximum((number + (BLOCK - 1)) // BLOCK, 1)
    blocks = jnp.broadcast_to(blocks, (n_res, 128))
    lower = jnp.where(
        lax.broadcasted_iota(jnp.int32, (n_res, n_res), 1) < lax.broadcasted_iota(jnp.int32, (n_res, n_res), 0), 1.0, 0.0
    ).astype(jnp.bfloat16)
    first = jnp.dot(
        lower, blocks.astype(jnp.float32).astype(jnp.bfloat16), preferred_element_type=jnp.float32
    ).astype(jnp.int32)
    last_ref[...] = jnp.clip(first + blocks - 1, 0, n_blocks - 1)
    place = jnp.sum(hit * (rank + (first[:, :1] * BLOCK).astype(jnp.float32)), axis=0, keepdims=True) - 1.0
    place = place.astype(jnp.int32)
    chosen = jnp.where(lax.broadcasted_iota(jnp.int32, (slots, cap), 0) == place, 1.0, 0.0).astype(jnp.bfloat16)
    line = lax.broadcasted_iota(jnp.int32, (8, cap), 0)
    values = jnp.where(line == 0, task_ref[0:1, :] + 1, jnp.where(line == 1, task_ref[1:2, :], 0))
    picked = lax.dot_general(
        values.astype(jnp.float32).astype(jnp.bfloat16),
        chosen,
        (((1,), (1,)), ((), ())),
        preferred_element_type=jnp.float32,
    ).astype(jnp.int32)
    starts = jnp.sum(jnp.where(lax.broadcasted_iota(jnp.int32, (n_res, 128), 1) == first, 1, 0), axis=0, keepdims=True)
    keep = jnp.concatenate([1 - starts, jnp.zeros((1, slots - 128), jnp.int32)], axis=1)
    picked = jnp.clip(picked, 0, jnp.where(lax.broadcasted_iota(jnp.int32, (8, slots), 0) == 0, n_amps, n_fetched - 1))
    slot_ref[...] = jnp.where(lax.broadcasted_iota(jnp.int32, (8, slots), 0) == 2, keep, picked)


def main_kernel(
    n_group, n_member, n_blocks,
    request_hbm, task_hbm, count_hbm, amp_hbm, int_hbm, out_ref,
    request_ref, task_ref, count_ref, slot_vmem, last_vmem, slot_ref, last_ref, amps, ints, fetched, outgoing, wanted, running, half, half_in, pair, pair_in,
    local_sem, req_send, req_recv, tile_send, tile_recv, half_send, half_recv, pair_send, pair_recv,
):
    g = lax.axis_index("group")
    m = lax.axis_index("member")
    n_z = n_member // 2
    z, core = m // 2, m % 2
    fetch_cap = request_ref.shape[1]
    tile = amps.shape[1]
    amp_copy = pltpu.make_async_copy(amp_hbm, amps.at[pl.ds(1, amp_hbm.shape[0])], local_sem.at[0])
    int_copy = pltpu.make_async_copy(int_hbm, ints, local_sem.at[1])
    request_copy = pltpu.make_async_copy(request_hbm, request_ref, local_sem.at[2])
    task_copy = pltpu.make_async_copy(task_hbm, task_ref, local_sem.at[3])
    count_copy = pltpu.make_async_copy(count_hbm, count_ref, local_sem.at[4])
    for copy in (request_copy, int_copy, task_copy, count_copy, amp_copy):
        copy.start()
    group_peers = [((g + i) % n_group, m) for i in range(1, n_group)]
    sibling = (g, z * 2 + 1 - core)
    z_peers = [(g, ((z + i) % n_z) * 2 + core) for i in range(1, n_z)]

    barrier = pltpu.get_barrier_semaphore()
    for peer in group_peers + [sibling] + z_peers:
        pl.semaphore_signal(barrier, inc=1, device_id=peer, device_id_type=MESH)
    amps[0] = jnp.zeros((tile, tile), amps.dtype)
    request_copy.wait()
    pl.semaphore_wait(barrier, n_group + n_z - 1)

    asks = []
    for i, peer in enumerate(group_peers):
        ask = pltpu.make_async_remote_copy(
            src_ref=request_ref, dst_ref=wanted.at[i], send_sem=req_send.at[i], recv_sem=req_recv.at[i],
            device_id=peer, device_id_type=MESH,
        )
        ask.start()
        asks.append(ask)
    int_copy.wait()
    for c in range(fetch_cap):
        fetched[g * fetch_cap + c] = ints[request_ref[g, c]]
    sends = []
    for i in range(n_group - 1):
        asks[i].wait_recv()
        for c in range(fetch_cap):
            outgoing[i, c] = ints[wanted[i, g, c]]
        send = pltpu.make_async_remote_copy(
            src_ref=outgoing.at[i], dst_ref=fetched.at[pl.ds(g * fetch_cap, fetch_cap)],
            send_sem=tile_send.at[i], recv_sem=tile_recv.at[i],
            device_id=((g + n_group - i - 1) % n_group, m), device_id_type=MESH,
        )
        send.start()
        sends.append(send)
    count_copy.wait()
    task_copy.wait()
    sort_tasks(
        n_member * RES_DEV, n_blocks, amp_hbm.shape[0], fetched.shape[0], count_ref[0], task_ref, slot_vmem, last_vmem,
    )
    slot_copy = pltpu.make_async_copy(slot_vmem, slot_ref, local_sem.at[5])
    last_copy = pltpu.make_async_copy(last_vmem, last_ref, local_sem.at[6])
    slot_copy.start()
    last_copy.start()
    amp_copy.wait()
    slot_copy.wait()
    last_copy.wait()
    for i in range(n_group - 1):
        asks[i].wait_send()
        source = (g + i + 1) % n_group
        pltpu.make_async_remote_copy(
            src_ref=outgoing.at[i], dst_ref=fetched.at[pl.ds(source * fetch_cap, fetch_cap)],
            send_sem=tile_send.at[i], recv_sem=tile_recv.at[i],
            device_id=group_peers[i], device_id_type=MESH,
        ).wait_recv()

    def block(b, total):
        for u in range(UNROLL):
            total = one_block(b * UNROLL + u, total)
        return total

    def one_block(b, total):
        left = []
        right = []
        for t in range(BLOCK):
            left.append(amps[slot_ref[0, b * BLOCK + t]])
            right.append(fetched[slot_ref[1, b * BLOCK + t]])
        product = jnp.dot(
            jnp.concatenate(left, axis=1), jnp.concatenate(right, axis=0), preferred_element_type=jnp.float32
        )
        total = jnp.where(slot_ref[2, b] != 0, total, 0.0) + product
        running[b] = total
        return total

    lax.fori_loop(0, n_blocks // UNROLL, block, jnp.zeros((tile, tile), jnp.float32))

    for k in range(n_z):
        half[k] = running[last_ref[2 * k + 1 - core, 0]]
    swap = pltpu.make_async_remote_copy(
        src_ref=half, dst_ref=half_in, send_sem=half_send, recv_sem=half_recv,
        device_id=sibling, device_id_type=MESH,
    )
    swap.start()
    swap.wait_recv()
    parts = []
    for i in range(1, n_z):
        k = (z + i) % n_z
        pair[i - 1] = running[last_ref[2 * k + core, 0]] + half_in[k]
        part = pltpu.make_async_remote_copy(
            src_ref=pair.at[i - 1], dst_ref=pair_in.at[i - 1],
            send_sem=pair_send.at[i - 1], recv_sem=pair_recv.at[i - 1],
            device_id=z_peers[i - 1], device_id_type=MESH,
        )
        part.start()
        parts.append(part)
    result = running[last_ref[m, 0]] + half_in[z]
    for i in range(n_z - 1):
        parts[i].wait_recv()
        result = result + pair_in[i]
    out_ref[0] = result
    swap.wait_send()
    for copy in sends + parts:
        copy.wait_send()


def sorted_tasks_call(amplitudes, integrals, tasks, requests, counts):
    tile = amplitudes.shape[1]
    n_group = lax.axis_size("group")
    n_member = lax.axis_size("member")
    n_res = RES_DEV * n_member
    cap = tasks.shape[0]
    fetch_cap = requests.shape[1]
    n_z = n_member // 2
    n_blocks = round_up((cap + BLOCK - 1) // BLOCK + n_res, UNROLL)
    slots = round_up(n_blocks * BLOCK, 128)
    vmem = pl.BlockSpec(memory_space=pltpu.VMEM)
    hbm = pl.BlockSpec(memory_space=pltpu.HBM)
    f32, bf16 = jnp.float32, amplitudes.dtype
    dma = pltpu.SemaphoreType.DMA
    return pl.pallas_call(
        functools.partial(main_kernel, n_group, n_member, n_blocks),
        out_shape=jax.ShapeDtypeStruct((RES_DEV, tile, tile), f32),
        in_specs=[hbm] * 5,
        out_specs=vmem,
        scratch_shapes=[
            pltpu.SMEM(requests.shape, jnp.int32),
            pltpu.VMEM((tasks.shape[1], cap), jnp.int32),
            pltpu.SMEM(counts.shape, jnp.int32),
            pltpu.VMEM((8, slots), jnp.int32),
            pltpu.VMEM((n_res, 128), jnp.int32),
            pltpu.SMEM((8, slots), jnp.int32),
            pltpu.SMEM((n_res, 128), jnp.int32),
            pltpu.VMEM((amplitudes.shape[0] + 1, tile, tile), bf16),
            pltpu.VMEM(integrals.shape, bf16),
            pltpu.VMEM((n_group * fetch_cap, tile, tile), bf16),
            pltpu.VMEM((n_group - 1, fetch_cap, tile, tile), bf16),
            pltpu.SMEM((n_group - 1,) + requests.shape, jnp.int32),
            pltpu.VMEM((n_blocks, tile, tile), f32),
            pltpu.VMEM((n_z, tile, tile), f32),
            pltpu.VMEM((n_z, tile, tile), f32),
            pltpu.VMEM((n_z - 1, tile, tile), f32),
            pltpu.VMEM((n_z - 1, tile, tile), f32),
            dma((7,)),
            dma((n_group - 1,)),
            dma((n_group - 1,)),
            dma((n_group - 1,)),
            dma((n_group - 1,)),
            dma,
            dma,
            dma((n_z - 1,)),
            dma((n_z - 1,)),
        ],
        compiler_params=pltpu.CompilerParams(
            collective_id=0, has_side_effects=True, vmem_limit_bytes=67043328
        ),
    )(requests, tasks.T, counts, amplitudes, integrals)


SUB = 8
CODES = 32767.0


def count_weights(n_bins, n_res, n_amps, parts, count, task_ref, e_ref, row_ref):
    cap = task_ref.shape[1]
    width = parts * n_amps * SUB
    share = -(-cap // parts)
    bins = task_ref[1:2, :] * n_res + task_ref[2:3, :]
    lane = lax.broadcasted_iota(jnp.int32, (1, cap), 1)
    amp = task_ref[0:1, :]
    for p in range(1, parts):
        amp = amp + jnp.where(lane >= p * share, n_amps, 0)
    hit_bin = (lax.broadcasted_iota(jnp.int32, (n_bins, cap), 0) == bins) & (
        lax.broadcasted_iota(jnp.int32, (n_bins, cap), 1) < count
    )
    first = amp * SUB
    rows = lax.broadcasted_iota(jnp.int32, (width, cap), 0)
    hit_amp = (rows >= first) & (rows < first + SUB)
    row_ref[...] = lax.dot_general(
        jnp.where(hit_bin, 1.0, 0.0).astype(jnp.bfloat16),
        jnp.where(hit_amp, 1.0, 0.0).astype(jnp.bfloat16),
        (((1,), (1,)), ((), ())),
        preferred_element_type=jnp.float32,
    )
    same = jnp.where(
        lax.broadcasted_iota(jnp.int32, (SUB, width), 1) % SUB
        == lax.broadcasted_iota(jnp.int32, (SUB, width), 0),
        1.0, 0.0,
    )
    for b in range(0, n_bins, 2):
        pair = [jnp.broadcast_to(row_ref[b + t:b + t + 1, :], (SUB, width)) * same for t in range(2)]
        e_ref[b * SUB:(b + 2) * SUB, :] = jnp.concatenate(pair, axis=0).astype(jnp.bfloat16)


def combine_amps(first, end, n_group, n_res, fetch_cap, parts, amps, e_ref, hi_ref, lo_ref):
    n_amps, tile = amps.shape[0], amps.shape[1]
    block = fetch_cap * n_res * SUB

    def rows16(q, carry):
        base = pl.multiple_of(q * 2 * SUB, 2 * SUB)
        rows = amps[:, pl.ds(base, 2 * SUB), :].astype(jnp.float32)
        halves = [
            rows[:, t * SUB:(t + 1) * SUB, :].reshape(n_amps * SUB, tile).astype(jnp.bfloat16) for t in range(2)
        ]
        right = jnp.concatenate(halves, axis=1)
        right = jnp.concatenate([right] * parts, axis=0)
        for h in range(n_group):
            made = jnp.dot(e_ref[h * block:(h + 1) * block, :], right, preferred_element_type=jnp.float32)
            for c in range(fetch_cap):
                for r in range(n_res):
                    at = (c * n_res + r) * SUB
                    value = jnp.concatenate(
                        [made[at:at + SUB, :tile], made[at:at + SUB, tile:]], axis=0
                    )
                    high = value.astype(jnp.bfloat16)
                    low = (value - high.astype(jnp.float32)).astype(jnp.bfloat16)
                    place = (h, pl.ds(pl.multiple_of(r * tile + base, 2 * SUB), 2 * SUB), pl.ds(c * tile, tile))
                    hi_ref[place] = high
                    lo_ref[place] = low
        return carry

    [rows16(q, 0) for q in range(first, end)]


def dense_kernel(
    n_group, n_member, parts,
    request_hbm, task_hbm, count_ref, amp_hbm, int_hbm, out_ref,
    request_ref, task_ref, amps, ints, fetched, outgoing, wanted, row_ref, e_ref, hi_ref, lo_ref, acc,
    half, half_in, code, code_in, scale, scale_in,
    local_sem, far_sem, chain_sem, req_send, req_recv, tile_send, tile_recv, half_send, half_recv,
    code_send, code_recv, scale_send, scale_recv,
):
    g = lax.axis_index("group")
    m = lax.axis_index("member")
    n_z = n_member // 2
    n_res = n_member * RES_DEV
    z, core = m // 2, m % 2
    fetch_cap = request_ref.shape[1]
    tile = amps.shape[1]
    amp_copy = pltpu.make_async_copy(amp_hbm, amps, local_sem.at[0])
    int_copy = pltpu.make_async_copy(int_hbm, ints, local_sem.at[1])
    request_copy = pltpu.make_async_copy(request_hbm, request_ref, local_sem.at[2])
    task_copy = pltpu.make_async_copy(task_hbm, task_ref, local_sem.at[3])
    for copy in (request_copy, int_copy, task_copy, amp_copy):
        copy.start()
    row, col = g // 2, g % 2
    near = [row * 2 + 1 - col, (1 - row) * 2 + col]
    partners = near + [(1 - row) * 2 + 1 - col]
    sibling = (g, z * 2 + 1 - core)

    barrier = pltpu.get_barrier_semaphore()

    def greet(device):
        pl.semaphore_signal(barrier, inc=1, device_id=device, device_id_type=MESH)

    for h in near:
        greet((h, m))
    greet(sibling)

    @pl.when(z > 0)
    def _():
        greet((g, m - 2))

    @pl.when(z < n_z - 1)
    def _():
        greet((g, m + 2))

    request_copy.wait()
    ends = jnp.where(z > 0, 1, 0) + jnp.where(z < n_z - 1, 1, 0)
    pl.semaphore_wait(barrier, 3 + ends)

    def ask(i):
        return pltpu.make_async_remote_copy(
            src_ref=request_ref, dst_ref=wanted.at[i], send_sem=req_send.at[i], recv_sem=req_recv.at[i],
            device_id=(partners[i], m), device_id_type=MESH,
        )

    def tiles(i, first=0, end=fetch_cap, slot=None):
        slot = i if slot is None else slot
        part = pl.ds(first, end - first)
        return pltpu.make_async_remote_copy(
            src_ref=outgoing.at[i, part], dst_ref=fetched.at[i + 1, part],
            send_sem=tile_send.at[slot], recv_sem=tile_recv.at[slot],
            device_id=(partners[i], m), device_id_type=MESH,
        )

    far = n_group - 2
    split = fetch_cap // 2
    pieces = [tiles(i) for i in range(far)] + [tiles(far, 0, split), tiles(far, split, fetch_cap, far + 1)]

    ask(0).start()
    ask(1).start()
    pl.semaphore_signal(far_sem, inc=1, device_id=(near[0], m), device_id_type=MESH)
    up, down = chain_sem.at[0], chain_sem.at[1]

    def tell_up():
        pl.semaphore_signal(up, inc=1, device_id=(g, m + 2), device_id_type=MESH)

    def tell_down():
        pl.semaphore_signal(down, inc=1, device_id=(g, m - 2), device_id_type=MESH)

    @pl.when((z == 1) & (z < n_z - 1))
    def _():
        tell_up()

    @pl.when((z == n_z - 2) & (z > 0))
    def _():
        tell_down()

    task_copy.wait()
    n_bins = n_group * fetch_cap * n_res
    count_weights(n_bins, n_res, amp_hbm.shape[0], parts, count_ref[0], task_ref, e_ref, row_ref)
    amp_copy.wait()
    steps = tile // (2 * SUB)
    early, middle = steps * 0 // 8, steps * 2 // 8

    def combine(first, end):
        combine_amps(first, end, n_group, n_res, fetch_cap, parts, amps, e_ref, hi_ref, lo_ref)

    combine(0, early)
    pl.semaphore_wait(far_sem, 1)
    ask(2).start()
    combine(early, middle)
    int_copy.wait()
    for c in range(fetch_cap):
        fetched[0, c] = ints[request_ref[g, c]]
    for i in range(n_group - 1):
        ask(i).wait_recv()
        for c in range(fetch_cap):
            outgoing[i, c] = ints[wanted[i, g, c]]
        for piece in pieces[i:i + 1] if i < far else pieces[far:]:
            piece.start()

    combine(middle, steps)

    @pl.when((z > 1) & (z < n_z - 1))
    def _():
        pl.semaphore_wait(up, 1)
        tell_up()

    @pl.when((z < n_z - 2) & (z > 0))
    def _():
        pl.semaphore_wait(down, 1)
        tell_down()

    def product(i, r, first, end):
        h = g if i == 0 else partners[i - 1]
        place = (h, pl.ds(pl.multiple_of(r * tile, tile), tile), pl.ds(first * tile, (end - first) * tile))
        right = fetched[i, first:end].reshape((end - first) * tile, tile)
        return jnp.dot(hi_ref[place], right, preferred_element_type=jnp.float32) + jnp.dot(
            lo_ref[place], right, preferred_element_type=jnp.float32
        )

    for i in range(n_group - 1):
        if i > 0:
            pieces[i - 1].wait_recv()

        for r in range(n_res):
            value = product(i, r, 0, fetch_cap)
            acc[r] = value if i == 0 else acc[r] + value
    last = n_group - 1
    pieces[far].wait_recv()
    for r in range(n_res):
        acc[r] = acc[r] + product(last, r, 0, split)

    low_end = z < n_z // 2

    def order(t):
        down_v = n_z - 1 - t
        down_k = jnp.where(down_v > z, down_v, down_v - 1)
        up_k = jnp.where(t < z, t, t + 1)
        return jnp.where(low_end, down_k, up_k)

    def swap(k):
        return pltpu.make_async_remote_copy(
            src_ref=half.at[k], dst_ref=half_in.at[k], send_sem=half_send.at[k], recv_sem=half_recv.at[k],
            device_id=sibling, device_id_type=MESH,
        )

    ks = [order(t) for t in range(n_z - 1)] + [z]
    @pl.when((z > 1) & (z == n_z - 1))
    def _():
        pl.semaphore_wait(up, 1)

    @pl.when((z < n_z - 2) & (z == 0))
    def _():
        pl.semaphore_wait(down, 1)

    pieces[far + 1].wait_recv()
    for k in ks:
        r = 2 * k + 1 - core
        half[k] = acc[r] + product(last, r, split, fetch_cap)
    for k in ks:
        swap(k).start()
    for k in ks:
        r = 2 * k + core
        acc[r] = acc[r] + product(last, r, split, fetch_cap)

    def sends(k):
        return [
            pltpu.make_async_remote_copy(
                src_ref=s.at[k], dst_ref=d.at[z], send_sem=ss.at[k], recv_sem=rs.at[z],
                device_id=(g, 2 * k + core), device_id_type=MESH,
            )
            for s, d, ss, rs in (
                (scale, scale_in, scale_send, scale_recv), (code, code_in, code_send, code_recv),
            )
        ]

    def arrivals(k):
        return [
            pltpu.make_async_remote_copy(
                src_ref=s.at[k], dst_ref=d.at[k], send_sem=ss.at[k], recv_sem=rs.at[k],
                device_id=(g, 2 * k + core), device_id_type=MESH,
            )
            for s, d, ss, rs in (
                (scale, scale_in, scale_send, scale_recv), (code, code_in, code_send, code_recv),
            )
        ]

    for k in ks[:-1]:
        swap(k).wait_recv()
        value = acc[2 * k + core] + half_in[k]
        top = jnp.maximum(jnp.max(jnp.abs(value), axis=0, keepdims=True), 1e-30)
        scale[k] = jnp.broadcast_to(top * (1.0 / CODES), (SUB, tile))
        code[k] = jnp.round(value * (CODES / top)).astype(jnp.int32).astype(jnp.int16)
        for copy in sends(k):
            copy.start()
    swap(z).wait_recv()
    result = acc[m] + half_in[z]
    for k in reversed(ks[:-1]):
        for copy in arrivals(k):
            copy.wait_recv()
        part = code_in[k].astype(jnp.int32).astype(jnp.float32)
        result = result + part * scale_in[k][:1, :]
    out_ref[0] = result
    for i in range(n_group - 1):
        ask(i).wait_send()
    for piece in pieces:
        piece.wait_send()
    for k in ks:
        swap(k).wait_send()
    for k in ks[:-1]:
        for copy in sends(k):
            copy.wait_send()


def dense_call(amplitudes, integrals, tasks, requests, counts):
    n_amps, tile = amplitudes.shape[0], amplitudes.shape[1]
    pin = functools.partial(pltpu.with_memory_space_constraint, memory_space=pltpu.HBM)
    n_group = lax.axis_size("group")
    n_member = lax.axis_size("member")
    n_res = RES_DEV * n_member
    n_z = n_member // 2
    cap = tasks.shape[0]
    fetch_cap = requests.shape[1]
    n_bins = n_group * fetch_cap * n_res
    parts = -(-cap // 256)
    width = parts * n_amps * SUB
    vmem = pl.BlockSpec(memory_space=pltpu.VMEM)
    hbm = pl.BlockSpec(memory_space=pltpu.HBM)
    f32, bf16 = jnp.float32, amplitudes.dtype
    dma = pltpu.SemaphoreType.DMA
    return pl.pallas_call(
        functools.partial(dense_kernel, n_group, n_member, parts),
        out_shape=jax.ShapeDtypeStruct((RES_DEV, tile, tile), f32),
        in_specs=[hbm, hbm, pl.BlockSpec(memory_space=pltpu.SMEM), hbm, hbm],
        out_specs=vmem,
        scratch_shapes=[
            pltpu.SMEM(requests.shape, jnp.int32),
            pltpu.VMEM((tasks.shape[1], cap), jnp.int32),
            pltpu.VMEM(amplitudes.shape, bf16),
            pltpu.VMEM(integrals.shape, bf16),
            pltpu.VMEM((n_group, fetch_cap, tile, tile), bf16),
            pltpu.VMEM((n_group - 1, fetch_cap, tile, tile), bf16),
            pltpu.SMEM((n_group - 1,) + requests.shape, jnp.int32),
            pltpu.VMEM((n_bins, width), f32),
            pltpu.VMEM((n_bins * SUB, width), bf16),
            pltpu.VMEM((n_group, n_res * tile, fetch_cap * tile), bf16),
            pltpu.VMEM((n_group, n_res * tile, fetch_cap * tile), bf16),
            pltpu.VMEM((n_res, tile, tile), f32),
            pltpu.VMEM((n_z, tile, tile), f32),
            pltpu.VMEM((n_z, tile, tile), f32),
            pltpu.VMEM((n_z, tile, tile), jnp.int16),
            pltpu.VMEM((n_z, tile, tile), jnp.int16),
            pltpu.VMEM((n_z, SUB, tile), f32),
            pltpu.VMEM((n_z, SUB, tile), f32),
            dma((5,)),
            pltpu.SemaphoreType.REGULAR,
            pltpu.SemaphoreType.REGULAR((2,)),
            dma((n_group - 1,)),
            dma((n_group - 1,)),
            dma((n_group,)),
            dma((n_group,)),
            dma((n_z,)),
            dma((n_z,)),
            dma((n_z,)),
            dma((n_z,)),
            dma((n_z,)),
            dma((n_z,)),
        ],
        compiler_params=pltpu.CompilerParams(
            collective_id=0, has_side_effects=True, vmem_limit_bytes=50331648
        ),
    )(pin(requests), pin(tasks.T), counts, pin(amplitudes), pin(integrals))


def per_device(amplitudes, integrals, tasks, requests, counts):
    n_bins = lax.axis_size("group") * requests.shape[1] * lax.axis_size("member") * RES_DEV
    if lax.axis_size("group") == 4 and n_bins * 2 <= tasks.shape[0]:
        return dense_call(amplitudes, integrals, tasks, requests, counts)
    return sorted_tasks_call(amplitudes, integrals, tasks, requests, counts)


def solution(mesh):
    return jax.shard_map(
        per_device,
        mesh=mesh,
        in_specs=(
            P(("group", "member"), None, None),
            P(("group", "member"), None, None),
            P(("group", "member"), None),
            P(("group", "member"), None),
            P(("group", "member")),
        ),
        out_specs=P(("group", "member"), None, None),
        check_vma=False,
    )
```

```python
import functools

import jax
import jax.numpy as jnp
from jax import lax
from jax.experimental import pallas as pl
from jax.experimental.pallas import tpu as pltpu
from jax.sharding import PartitionSpec as P

RES_DEV = 1
BLOCK = 8
UNROLL = 8
MESH = pl.DeviceIdType.MESH


def round_up(n, k):
    return (n + k - 1) // k * k


def sort_tasks(n_res, n_blocks, n_amps, n_fetched, count, task_ref, slot_ref, last_ref):
    cap = task_ref.shape[1]
    slots = slot_ref.shape[1]
    valid = lax.broadcasted_iota(jnp.int32, (n_res, cap), 1) < count
    rows = lax.broadcasted_iota(jnp.int32, (n_res, cap), 0)
    hit = jnp.where(valid & (rows == task_ref[2:3, :]), 1.0, 0.0)
    upper = jnp.where(
        lax.broadcasted_iota(jnp.int32, (cap, cap), 0) <= lax.broadcasted_iota(jnp.int32, (cap, cap), 1), 1.0, 0.0
    ).astype(jnp.bfloat16)
    rank = jnp.dot(hit.astype(jnp.bfloat16), upper, preferred_element_type=jnp.float32)
    number = jnp.sum(hit, axis=1, keepdims=True).astype(jnp.int32)
    blocks = jnp.maximum((number + (BLOCK - 1)) // BLOCK, 1)
    blocks = jnp.broadcast_to(blocks, (n_res, 128))
    lower = jnp.where(
        lax.broadcasted_iota(jnp.int32, (n_res, n_res), 1) < lax.broadcasted_iota(jnp.int32, (n_res, n_res), 0), 1.0, 0.0
    ).astype(jnp.bfloat16)
    first = jnp.dot(
        lower, blocks.astype(jnp.float32).astype(jnp.bfloat16), preferred_element_type=jnp.float32
    ).astype(jnp.int32)
    last_ref[...] = jnp.clip(first + blocks - 1, 0, n_blocks - 1)
    place = jnp.sum(hit * (rank + (first[:, :1] * BLOCK).astype(jnp.float32)), axis=0, keepdims=True) - 1.0
    place = place.astype(jnp.int32)
    chosen = jnp.where(lax.broadcasted_iota(jnp.int32, (slots, cap), 0) == place, 1.0, 0.0).astype(jnp.bfloat16)
    line = lax.broadcasted_iota(jnp.int32, (8, cap), 0)
    values = jnp.where(line == 0, task_ref[0:1, :] + 1, jnp.where(line == 1, task_ref[1:2, :], 0))
    picked = lax.dot_general(
        values.astype(jnp.float32).astype(jnp.bfloat16),
        chosen,
        (((1,), (1,)), ((), ())),
        preferred_element_type=jnp.float32,
    ).astype(jnp.int32)
    starts = jnp.sum(jnp.where(lax.broadcasted_iota(jnp.int32, (n_res, 128), 1) == first, 1, 0), axis=0, keepdims=True)
    keep = jnp.concatenate([1 - starts, jnp.zeros((1, slots - 128), jnp.int32)], axis=1)
    picked = jnp.clip(picked, 0, jnp.where(lax.broadcasted_iota(jnp.int32, (8, slots), 0) == 0, n_amps, n_fetched - 1))
    slot_ref[...] = jnp.where(lax.broadcasted_iota(jnp.int32, (8, slots), 0) == 2, keep, picked)


def main_kernel(
    n_group, n_member, n_blocks,
    request_hbm, task_hbm, count_hbm, amp_hbm, int_hbm, out_ref,
    request_ref, task_ref, count_ref, slot_vmem, last_vmem, slot_ref, last_ref, amps, ints, fetched, outgoing, wanted, running, half, half_in, pair, pair_in,
    local_sem, req_send, req_recv, tile_send, tile_recv, half_send, half_recv, pair_send, pair_recv,
):
    g = lax.axis_index("group")
    m = lax.axis_index("member")
    n_z = n_member // 2
    z, core = m // 2, m % 2
    fetch_cap = request_ref.shape[1]
    tile = amps.shape[1]
    amp_copy = pltpu.make_async_copy(amp_hbm, amps.at[pl.ds(1, amp_hbm.shape[0])], local_sem.at[0])
    int_copy = pltpu.make_async_copy(int_hbm, ints, local_sem.at[1])
    request_copy = pltpu.make_async_copy(request_hbm, request_ref, local_sem.at[2])
    task_copy = pltpu.make_async_copy(task_hbm, task_ref, local_sem.at[3])
    count_copy = pltpu.make_async_copy(count_hbm, count_ref, local_sem.at[4])
    for copy in (request_copy, int_copy, task_copy, count_copy, amp_copy):
        copy.start()
    group_peers = [((g + i) % n_group, m) for i in range(1, n_group)]
    sibling = (g, z * 2 + 1 - core)
    z_peers = [(g, ((z + i) % n_z) * 2 + core) for i in range(1, n_z)]

    barrier = pltpu.get_barrier_semaphore()
    for peer in group_peers + [sibling] + z_peers:
        pl.semaphore_signal(barrier, inc=1, device_id=peer, device_id_type=MESH)
    amps[0] = jnp.zeros((tile, tile), amps.dtype)
    request_copy.wait()
    pl.semaphore_wait(barrier, n_group + n_z - 1)

    asks = []
    for i, peer in enumerate(group_peers):
        ask = pltpu.make_async_remote_copy(
            src_ref=request_ref, dst_ref=wanted.at[i], send_sem=req_send.at[i], recv_sem=req_recv.at[i],
            device_id=peer, device_id_type=MESH,
        )
        ask.start()
        asks.append(ask)
    int_copy.wait()
    for c in range(fetch_cap):
        fetched[g * fetch_cap + c] = ints[request_ref[g, c]]
    sends = []
    for i in range(n_group - 1):
        asks[i].wait_recv()
        for c in range(fetch_cap):
            outgoing[i, c] = ints[wanted[i, g, c]]
        send = pltpu.make_async_remote_copy(
            src_ref=outgoing.at[i], dst_ref=fetched.at[pl.ds(g * fetch_cap, fetch_cap)],
            send_sem=tile_send.at[i], recv_sem=tile_recv.at[i],
            device_id=((g + n_group - i - 1) % n_group, m), device_id_type=MESH,
        )
        send.start()
        sends.append(send)
    count_copy.wait()
    task_copy.wait()
    sort_tasks(
        n_member * RES_DEV, n_blocks, amp_hbm.shape[0], fetched.shape[0], count_ref[0], task_ref, slot_vmem, last_vmem,
    )
    slot_copy = pltpu.make_async_copy(slot_vmem, slot_ref, local_sem.at[5])
    last_copy = pltpu.make_async_copy(last_vmem, last_ref, local_sem.at[6])
    slot_copy.start()
    last_copy.start()
    amp_copy.wait()
    slot_copy.wait()
    last_copy.wait()
    for i in range(n_group - 1):
        asks[i].wait_send()
        source = (g + i + 1) % n_group
        pltpu.make_async_remote_copy(
            src_ref=outgoing.at[i], dst_ref=fetched.at[pl.ds(source * fetch_cap, fetch_cap)],
            send_sem=tile_send.at[i], recv_sem=tile_recv.at[i],
            device_id=group_peers[i], device_id_type=MESH,
        ).wait_recv()

    def block(b, total):
        for u in range(UNROLL):
            total = one_block(b * UNROLL + u, total)
        return total

    def one_block(b, total):
        left = []
        right = []
        for t in range(BLOCK):
            left.append(amps[slot_ref[0, b * BLOCK + t]])
            right.append(fetched[slot_ref[1, b * BLOCK + t]])
        product = jnp.dot(
            jnp.concatenate(left, axis=1), jnp.concatenate(right, axis=0), preferred_element_type=jnp.float32
        )
        total = jnp.where(slot_ref[2, b] != 0, total, 0.0) + product
        running[b] = total
        return total

    lax.fori_loop(0, n_blocks // UNROLL, block, jnp.zeros((tile, tile), jnp.float32))

    for k in range(n_z):
        half[k] = running[last_ref[2 * k + 1 - core, 0]]
    swap = pltpu.make_async_remote_copy(
        src_ref=half, dst_ref=half_in, send_sem=half_send, recv_sem=half_recv,
        device_id=sibling, device_id_type=MESH,
    )
    swap.start()
    swap.wait_recv()
    parts = []
    for i in range(1, n_z):
        k = (z + i) % n_z
        pair[i - 1] = running[last_ref[2 * k + core, 0]] + half_in[k]
        part = pltpu.make_async_remote_copy(
            src_ref=pair.at[i - 1], dst_ref=pair_in.at[i - 1],
            send_sem=pair_send.at[i - 1], recv_sem=pair_recv.at[i - 1],
            device_id=z_peers[i - 1], device_id_type=MESH,
        )
        part.start()
        parts.append(part)
    result = running[last_ref[m, 0]] + half_in[z]
    for i in range(n_z - 1):
        parts[i].wait_recv()
        result = result + pair_in[i]
    out_ref[0] = result
    swap.wait_send()
    for copy in sends + parts:
        copy.wait_send()


def sorted_tasks_call(amplitudes, integrals, tasks, requests, counts):
    tile = amplitudes.shape[1]
    n_group = lax.axis_size("group")
    n_member = lax.axis_size("member")
    n_res = RES_DEV * n_member
    cap = tasks.shape[0]
    fetch_cap = requests.shape[1]
    n_z = n_member // 2
    n_blocks = round_up((cap + BLOCK - 1) // BLOCK + n_res, UNROLL)
    slots = round_up(n_blocks * BLOCK, 128)
    vmem = pl.BlockSpec(memory_space=pltpu.VMEM)
    hbm = pl.BlockSpec(memory_space=pltpu.HBM)
    f32, bf16 = jnp.float32, amplitudes.dtype
    dma = pltpu.SemaphoreType.DMA
    return pl.pallas_call(
        functools.partial(main_kernel, n_group, n_member, n_blocks),
        out_shape=jax.ShapeDtypeStruct((RES_DEV, tile, tile), f32),
        in_specs=[hbm] * 5,
        out_specs=vmem,
        scratch_shapes=[
            pltpu.SMEM(requests.shape, jnp.int32),
            pltpu.VMEM((tasks.shape[1], cap), jnp.int32),
            pltpu.SMEM(counts.shape, jnp.int32),
            pltpu.VMEM((8, slots), jnp.int32),
            pltpu.VMEM((n_res, 128), jnp.int32),
            pltpu.SMEM((8, slots), jnp.int32),
            pltpu.SMEM((n_res, 128), jnp.int32),
            pltpu.VMEM((amplitudes.shape[0] + 1, tile, tile), bf16),
            pltpu.VMEM(integrals.shape, bf16),
            pltpu.VMEM((n_group * fetch_cap, tile, tile), bf16),
            pltpu.VMEM((n_group - 1, fetch_cap, tile, tile), bf16),
            pltpu.SMEM((n_group - 1,) + requests.shape, jnp.int32),
            pltpu.VMEM((n_blocks, tile, tile), f32),
            pltpu.VMEM((n_z, tile, tile), f32),
            pltpu.VMEM((n_z, tile, tile), f32),
            pltpu.VMEM((n_z - 1, tile, tile), f32),
            pltpu.VMEM((n_z - 1, tile, tile), f32),
            dma((7,)),
            dma((n_group - 1,)),
            dma((n_group - 1,)),
            dma((n_group - 1,)),
            dma((n_group - 1,)),
            dma,
            dma,
            dma((n_z - 1,)),
            dma((n_z - 1,)),
        ],
        compiler_params=pltpu.CompilerParams(
            collective_id=0, has_side_effects=True, vmem_limit_bytes=67043328
        ),
    )(requests, tasks.T, counts, amplitudes, integrals)


SUB = 8
CODES = 32767.0


def count_weights(n_bins, n_res, n_amps, parts, count, task_ref, e_ref, row_ref):
    cap = task_ref.shape[1]
    width = parts * n_amps * SUB
    share = -(-cap // parts)
    bins = task_ref[1:2, :] * n_res + task_ref[2:3, :]
    lane = lax.broadcasted_iota(jnp.int32, (1, cap), 1)
    amp = task_ref[0:1, :]
    for p in range(1, parts):
        amp = amp + jnp.where(lane >= p * share, n_amps, 0)
    hit_bin = (lax.broadcasted_iota(jnp.int32, (n_bins, cap), 0) == bins) & (
        lax.broadcasted_iota(jnp.int32, (n_bins, cap), 1) < count
    )
    first = amp * SUB
    rows = lax.broadcasted_iota(jnp.int32, (width, cap), 0)
    hit_amp = (rows >= first) & (rows < first + SUB)
    row_ref[...] = lax.dot_general(
        jnp.where(hit_bin, 1.0, 0.0).astype(jnp.bfloat16),
        jnp.where(hit_amp, 1.0, 0.0).astype(jnp.bfloat16),
        (((1,), (1,)), ((), ())),
        preferred_element_type=jnp.float32,
    )
    same = jnp.where(
        lax.broadcasted_iota(jnp.int32, (SUB, width), 1) % SUB
        == lax.broadcasted_iota(jnp.int32, (SUB, width), 0),
        1.0, 0.0,
    )
    for b in range(0, n_bins, 2):
        pair = [jnp.broadcast_to(row_ref[b + t:b + t + 1, :], (SUB, width)) * same for t in range(2)]
        e_ref[b * SUB:(b + 2) * SUB, :] = jnp.concatenate(pair, axis=0).astype(jnp.bfloat16)


def combine_amps(first, end, n_group, n_res, fetch_cap, parts, amps, e_ref, hi_ref, lo_ref):
    n_amps, tile = amps.shape[0], amps.shape[1]
    block = fetch_cap * n_res * SUB

    def rows16(q, carry):
        base = pl.multiple_of(q * 2 * SUB, 2 * SUB)
        rows = amps[:, pl.ds(base, 2 * SUB), :].astype(jnp.float32)
        halves = [
            rows[:, t * SUB:(t + 1) * SUB, :].reshape(n_amps * SUB, tile).astype(jnp.bfloat16) for t in range(2)
        ]
        right = jnp.concatenate(halves, axis=1)
        right = jnp.concatenate([right] * parts, axis=0)
        for h in range(n_group):
            made = jnp.dot(e_ref[h * block:(h + 1) * block, :], right, preferred_element_type=jnp.float32)
            for c in range(fetch_cap):
                for r in range(n_res):
                    at = (c * n_res + r) * SUB
                    value = jnp.concatenate(
                        [made[at:at + SUB, :tile], made[at:at + SUB, tile:]], axis=0
                    )
                    high = value.astype(jnp.bfloat16)
                    low = (value - high.astype(jnp.float32)).astype(jnp.bfloat16)
                    place = (h, pl.ds(pl.multiple_of(r * tile + base, 2 * SUB), 2 * SUB), pl.ds(c * tile, tile))
                    hi_ref[place] = high
                    lo_ref[place] = low
        return carry

    [rows16(q, 0) for q in range(first, end)]


def dense_kernel(
    n_group, n_member, parts,
    request_hbm, task_hbm, count_ref, amp_hbm, int_hbm, out_ref,
    request_ref, task_ref, amps, ints, fetched, outgoing, wanted, row_ref, e_ref, hi_ref, lo_ref, acc,
    half, half_in, code, code_in, scale, scale_in,
    local_sem, chain_sem, req_send, req_recv, tile_send, tile_recv, half_send, half_recv,
    code_send, code_recv, scale_send, scale_recv,
):
    g = lax.axis_index("group")
    m = lax.axis_index("member")
    n_z = n_member // 2
    n_res = n_member * RES_DEV
    z, core = m // 2, m % 2
    fetch_cap = request_ref.shape[1]
    tile = amps.shape[1]
    amp_copy = pltpu.make_async_copy(amp_hbm, amps, local_sem.at[0])
    int_copy = pltpu.make_async_copy(int_hbm, ints, local_sem.at[1])
    request_copy = pltpu.make_async_copy(request_hbm, request_ref, local_sem.at[2])
    task_copy = pltpu.make_async_copy(task_hbm, task_ref, local_sem.at[3])
    for copy in (request_copy, int_copy, task_copy, amp_copy):
        copy.start()
    row, col = g // 2, g % 2
    near = [row * 2 + 1 - col, (1 - row) * 2 + col]
    partners = near + [(1 - row) * 2 + 1 - col]
    sibling = (g, z * 2 + 1 - core)

    barrier = pltpu.get_barrier_semaphore()

    def greet(device):
        pl.semaphore_signal(barrier, inc=1, device_id=device, device_id_type=MESH)

    for h in partners:
        greet((h, m))
    greet(sibling)

    @pl.when(z > 0)
    def _():
        greet((g, m - 2))

    @pl.when(z < n_z - 1)
    def _():
        greet((g, m + 2))

    request_copy.wait()
    ends = jnp.where(z > 0, 1, 0) + jnp.where(z < n_z - 1, 1, 0)
    pl.semaphore_wait(barrier, n_group + ends)

    def ask(i):
        return pltpu.make_async_remote_copy(
            src_ref=request_ref, dst_ref=wanted.at[i], send_sem=req_send.at[i], recv_sem=req_recv.at[i],
            device_id=(partners[i], m), device_id_type=MESH,
        )

    def tiles(i, first=0, end=fetch_cap, slot=None):
        slot = i if slot is None else slot
        part = pl.ds(first, end - first)
        return pltpu.make_async_remote_copy(
            src_ref=outgoing.at[i, part], dst_ref=fetched.at[i + 1, part],
            send_sem=tile_send.at[slot], recv_sem=tile_recv.at[slot],
            device_id=(partners[i], m), device_id_type=MESH,
        )

    far = n_group - 2
    split = fetch_cap // 2
    pieces = [tiles(i) for i in range(far)] + [tiles(far, 0, split), tiles(far, split, fetch_cap, far + 1)]

    ask(0).start()
    ask(1).start()
    ask(2).start()
    up, down = chain_sem.at[0], chain_sem.at[1]

    def tell_up():
        pl.semaphore_signal(up, inc=1, device_id=(g, m + 2), device_id_type=MESH)

    def tell_down():
        pl.semaphore_signal(down, inc=1, device_id=(g, m - 2), device_id_type=MESH)

    @pl.when((z == 1) & (z < n_z - 1))
    def _():
        tell_up()

    @pl.when((z == n_z - 2) & (z > 0))
    def _():
        tell_down()

    task_copy.wait()
    n_bins = n_group * fetch_cap * n_res
    count_weights(n_bins, n_res, amp_hbm.shape[0], parts, count_ref[0], task_ref, e_ref, row_ref)
    amp_copy.wait()
    steps = tile // (2 * SUB)
    early, middle = steps * 0 // 8, steps * 2 // 8

    def combine(first, end):
        combine_amps(first, end, n_group, n_res, fetch_cap, parts, amps, e_ref, hi_ref, lo_ref)

    combine(0, early)
    combine(early, middle)
    int_copy.wait()
    for c in range(fetch_cap):
        fetched[0, c] = ints[request_ref[g, c]]
    for i in range(n_group - 1):
        ask(i).wait_recv()
        for c in range(fetch_cap):
            outgoing[i, c] = ints[wanted[i, g, c]]
        for piece in pieces[i:i + 1] if i < far else pieces[far:]:
            piece.start()

    combine(middle, steps)

    @pl.when((z > 1) & (z < n_z - 1))
    def _():
        pl.semaphore_wait(up, 1)
        tell_up()

    @pl.when((z < n_z - 2) & (z > 0))
    def _():
        pl.semaphore_wait(down, 1)
        tell_down()

    def product(i, r, first, end):
        h = g if i == 0 else partners[i - 1]
        place = (h, pl.ds(pl.multiple_of(r * tile, tile), tile), pl.ds(first * tile, (end - first) * tile))
        right = fetched[i, first:end].reshape((end - first) * tile, tile)
        return jnp.dot(hi_ref[place], right, preferred_element_type=jnp.float32) + jnp.dot(
            lo_ref[place], right, preferred_element_type=jnp.float32
        )

    for i in range(n_group - 1):
        if i > 0:
            pieces[i - 1].wait_recv()

        for r in range(n_res):
            value = product(i, r, 0, fetch_cap)
            acc[r] = value if i == 0 else acc[r] + value
    last = n_group - 1
    pieces[far].wait_recv()
    for r in range(n_res):
        acc[r] = acc[r] + product(last, r, 0, split)

    low_end = z < n_z // 2

    def order(t):
        down_v = n_z - 1 - t
        down_k = jnp.where(down_v > z, down_v, down_v - 1)
        up_k = jnp.where(t < z, t, t + 1)
        return jnp.where(low_end, down_k, up_k)

    def swap(k):
        return pltpu.make_async_remote_copy(
            src_ref=half.at[k], dst_ref=half_in.at[k], send_sem=half_send.at[k], recv_sem=half_recv.at[k],
            device_id=sibling, device_id_type=MESH,
        )

    ks = [order(t) for t in range(n_z - 1)] + [z]
    @pl.when((z > 1) & (z == n_z - 1))
    def _():
        pl.semaphore_wait(up, 1)

    @pl.when((z < n_z - 2) & (z == 0))
    def _():
        pl.semaphore_wait(down, 1)

    pieces[far + 1].wait_recv()
    for k in ks:
        r = 2 * k + 1 - core
        half[k] = acc[r] + product(last, r, split, fetch_cap)
    for k in ks:
        r = 2 * k + core
        acc[r] = acc[r] + product(last, r, split, fetch_cap)
    for k in ks:
        swap(k).start()

    def sends(k):
        return [
            pltpu.make_async_remote_copy(
                src_ref=s.at[k], dst_ref=d.at[z], send_sem=ss.at[k], recv_sem=rs.at[z],
                device_id=(g, 2 * k + core), device_id_type=MESH,
            )
            for s, d, ss, rs in (
                (scale, scale_in, scale_send, scale_recv), (code, code_in, code_send, code_recv),
            )
        ]

    def arrivals(k):
        return [
            pltpu.make_async_remote_copy(
                src_ref=s.at[k], dst_ref=d.at[k], send_sem=ss.at[k], recv_sem=rs.at[k],
                device_id=(g, 2 * k + core), device_id_type=MESH,
            )
            for s, d, ss, rs in (
                (scale, scale_in, scale_send, scale_recv), (code, code_in, code_send, code_recv),
            )
        ]

    for k in ks[:-1]:
        swap(k).wait_recv()
        value = acc[2 * k + core] + half_in[k]
        top = jnp.maximum(jnp.max(jnp.abs(value), axis=0, keepdims=True), 1e-30)
        scale[k] = top * (1.0 / CODES)
        code[k] = jnp.round(value * (CODES / top)).astype(jnp.int32).astype(jnp.int16)
        for copy in sends(k):
            copy.start()
    swap(z).wait_recv()
    result = acc[m] + half_in[z]
    for k in reversed(ks[:-1]):
        for copy in arrivals(k):
            copy.wait_recv()
        part = code_in[k].astype(jnp.int32).astype(jnp.float32)
        result = result + part * scale_in[k]
    out_ref[0] = result
    for i in range(n_group - 1):
        ask(i).wait_send()
    for piece in pieces:
        piece.wait_send()
    for k in ks:
        swap(k).wait_send()
    for k in ks[:-1]:
        for copy in sends(k):
            copy.wait_send()


def dense_call(amplitudes, integrals, tasks, requests, counts):
    n_amps, tile = amplitudes.shape[0], amplitudes.shape[1]
    pin = functools.partial(pltpu.with_memory_space_constraint, memory_space=pltpu.HBM)
    n_group = lax.axis_size("group")
    n_member = lax.axis_size("member")
    n_res = RES_DEV * n_member
    n_z = n_member // 2
    cap = tasks.shape[0]
    fetch_cap = requests.shape[1]
    n_bins = n_group * fetch_cap * n_res
    parts = -(-cap // 256)
    width = parts * n_amps * SUB
    vmem = pl.BlockSpec(memory_space=pltpu.VMEM)
    hbm = pl.BlockSpec(memory_space=pltpu.HBM)
    f32, bf16 = jnp.float32, amplitudes.dtype
    dma = pltpu.SemaphoreType.DMA
    return pl.pallas_call(
        functools.partial(dense_kernel, n_group, n_member, parts),
        out_shape=jax.ShapeDtypeStruct((RES_DEV, tile, tile), f32),
        in_specs=[hbm, hbm, pl.BlockSpec(memory_space=pltpu.SMEM), hbm, hbm],
        out_specs=vmem,
        scratch_shapes=[
            pltpu.SMEM(requests.shape, jnp.int32),
            pltpu.VMEM((tasks.shape[1], cap), jnp.int32),
            pltpu.VMEM(amplitudes.shape, bf16),
            pltpu.VMEM(integrals.shape, bf16),
            pltpu.VMEM((n_group, fetch_cap, tile, tile), bf16),
            pltpu.VMEM((n_group - 1, fetch_cap, tile, tile), bf16),
            pltpu.SMEM((n_group - 1,) + requests.shape, jnp.int32),
            pltpu.VMEM((n_bins, width), f32),
            pltpu.VMEM((n_bins * SUB, width), bf16),
            pltpu.VMEM((n_group, n_res * tile, fetch_cap * tile), bf16),
            pltpu.VMEM((n_group, n_res * tile, fetch_cap * tile), bf16),
            pltpu.VMEM((n_res, tile, tile), f32),
            pltpu.VMEM((n_z, tile, tile), f32),
            pltpu.VMEM((n_z, tile, tile), f32),
            pltpu.VMEM((n_z, tile, tile), jnp.int16),
            pltpu.VMEM((n_z, tile, tile), jnp.int16),
            pltpu.VMEM((n_z, 1, tile), f32),
            pltpu.VMEM((n_z, 1, tile), f32),
            dma((5,)),
            pltpu.SemaphoreType.REGULAR((2,)),
            dma((n_group - 1,)),
            dma((n_group - 1,)),
            dma((n_group,)),
            dma((n_group,)),
            dma((n_z,)),
            dma((n_z,)),
            dma((n_z,)),
            dma((n_z,)),
            dma((n_z,)),
            dma((n_z,)),
        ],
        compiler_params=pltpu.CompilerParams(
            collective_id=0, has_side_effects=True, vmem_limit_bytes=50331648
        ),
    )(pin(requests), pin(tasks.T), counts, pin(amplitudes), pin(integrals))


def per_device(amplitudes, integrals, tasks, requests, counts):
    n_bins = lax.axis_size("group") * requests.shape[1] * lax.axis_size("member") * RES_DEV
    if lax.axis_size("group") == 4 and n_bins * 2 <= tasks.shape[0]:
        return dense_call(amplitudes, integrals, tasks, requests, counts)
    return sorted_tasks_call(amplitudes, integrals, tasks, requests, counts)


def solution(mesh):
    return jax.shard_map(
        per_device,
        mesh=mesh,
        in_specs=(
            P(("group", "member"), None, None),
            P(("group", "member"), None, None),
            P(("group", "member"), None),
            P(("group", "member"), None),
            P(("group", "member")),
        ),
        out_specs=P(("group", "member"), None, None),
        check_vma=False,
    )
```

```python
import functools

import jax
import jax.numpy as jnp
from jax import lax
from jax.experimental import pallas as pl
from jax.experimental.pallas import tpu as pltpu
from jax.sharding import PartitionSpec as P

RES_DEV = 1
BLOCK = 8
UNROLL = 8
MESH = pl.DeviceIdType.MESH


def round_up(n, k):
    return (n + k - 1) // k * k


def sort_tasks(n_res, n_blocks, n_amps, n_fetched, count, task_ref, slot_ref, last_ref):
    cap = task_ref.shape[1]
    slots = slot_ref.shape[1]
    valid = lax.broadcasted_iota(jnp.int32, (n_res, cap), 1) < count
    rows = lax.broadcasted_iota(jnp.int32, (n_res, cap), 0)
    hit = jnp.where(valid & (rows == task_ref[2:3, :]), 1.0, 0.0)
    upper = jnp.where(
        lax.broadcasted_iota(jnp.int32, (cap, cap), 0) <= lax.broadcasted_iota(jnp.int32, (cap, cap), 1), 1.0, 0.0
    ).astype(jnp.bfloat16)
    rank = jnp.dot(hit.astype(jnp.bfloat16), upper, preferred_element_type=jnp.float32)
    number = jnp.sum(hit, axis=1, keepdims=True).astype(jnp.int32)
    blocks = jnp.maximum((number + (BLOCK - 1)) // BLOCK, 1)
    blocks = jnp.broadcast_to(blocks, (n_res, 128))
    lower = jnp.where(
        lax.broadcasted_iota(jnp.int32, (n_res, n_res), 1) < lax.broadcasted_iota(jnp.int32, (n_res, n_res), 0), 1.0, 0.0
    ).astype(jnp.bfloat16)
    first = jnp.dot(
        lower, blocks.astype(jnp.float32).astype(jnp.bfloat16), preferred_element_type=jnp.float32
    ).astype(jnp.int32)
    last_ref[...] = jnp.clip(first + blocks - 1, 0, n_blocks - 1)
    place = jnp.sum(hit * (rank + (first[:, :1] * BLOCK).astype(jnp.float32)), axis=0, keepdims=True) - 1.0
    place = place.astype(jnp.int32)
    chosen = jnp.where(lax.broadcasted_iota(jnp.int32, (slots, cap), 0) == place, 1.0, 0.0).astype(jnp.bfloat16)
    line = lax.broadcasted_iota(jnp.int32, (8, cap), 0)
    values = jnp.where(line == 0, task_ref[0:1, :] + 1, jnp.where(line == 1, task_ref[1:2, :], 0))
    picked = lax.dot_general(
        values.astype(jnp.float32).astype(jnp.bfloat16),
        chosen,
        (((1,), (1,)), ((), ())),
        preferred_element_type=jnp.float32,
    ).astype(jnp.int32)
    starts = jnp.sum(jnp.where(lax.broadcasted_iota(jnp.int32, (n_res, 128), 1) == first, 1, 0), axis=0, keepdims=True)
    keep = jnp.concatenate([1 - starts, jnp.zeros((1, slots - 128), jnp.int32)], axis=1)
    picked = jnp.clip(picked, 0, jnp.where(lax.broadcasted_iota(jnp.int32, (8, slots), 0) == 0, n_amps, n_fetched - 1))
    slot_ref[...] = jnp.where(lax.broadcasted_iota(jnp.int32, (8, slots), 0) == 2, keep, picked)


def main_kernel(
    n_group, n_member, n_blocks,
    request_hbm, task_hbm, count_hbm, amp_hbm, int_hbm, out_ref,
    request_ref, task_ref, count_ref, slot_vmem, last_vmem, slot_ref, last_ref, amps, ints, fetched, outgoing, wanted, running, half, half_in, pair, pair_in,
    local_sem, req_send, req_recv, tile_send, tile_recv, half_send, half_recv, pair_send, pair_recv,
):
    g = lax.axis_index("group")
    m = lax.axis_index("member")
    n_z = n_member // 2
    z, core = m // 2, m % 2
    fetch_cap = request_ref.shape[1]
    tile = amps.shape[1]
    amp_copy = pltpu.make_async_copy(amp_hbm, amps.at[pl.ds(1, amp_hbm.shape[0])], local_sem.at[0])
    int_copy = pltpu.make_async_copy(int_hbm, ints, local_sem.at[1])
    request_copy = pltpu.make_async_copy(request_hbm, request_ref, local_sem.at[2])
    task_copy = pltpu.make_async_copy(task_hbm, task_ref, local_sem.at[3])
    count_copy = pltpu.make_async_copy(count_hbm, count_ref, local_sem.at[4])
    for copy in (request_copy, int_copy, task_copy, count_copy, amp_copy):
        copy.start()
    group_peers = [((g + i) % n_group, m) for i in range(1, n_group)]
    sibling = (g, z * 2 + 1 - core)
    z_peers = [(g, ((z + i) % n_z) * 2 + core) for i in range(1, n_z)]

    barrier = pltpu.get_barrier_semaphore()
    for peer in group_peers + [sibling] + z_peers:
        pl.semaphore_signal(barrier, inc=1, device_id=peer, device_id_type=MESH)
    amps[0] = jnp.zeros((tile, tile), amps.dtype)
    request_copy.wait()
    pl.semaphore_wait(barrier, n_group + n_z - 1)

    asks = []
    for i, peer in enumerate(group_peers):
        ask = pltpu.make_async_remote_copy(
            src_ref=request_ref, dst_ref=wanted.at[i], send_sem=req_send.at[i], recv_sem=req_recv.at[i],
            device_id=peer, device_id_type=MESH,
        )
        ask.start()
        asks.append(ask)
    int_copy.wait()
    for c in range(fetch_cap):
        fetched[g * fetch_cap + c] = ints[request_ref[g, c]]
    sends = []
    for i in range(n_group - 1):
        asks[i].wait_recv()
        for c in range(fetch_cap):
            outgoing[i, c] = ints[wanted[i, g, c]]
        send = pltpu.make_async_remote_copy(
            src_ref=outgoing.at[i], dst_ref=fetched.at[pl.ds(g * fetch_cap, fetch_cap)],
            send_sem=tile_send.at[i], recv_sem=tile_recv.at[i],
            device_id=((g + n_group - i - 1) % n_group, m), device_id_type=MESH,
        )
        send.start()
        sends.append(send)
    count_copy.wait()
    task_copy.wait()
    sort_tasks(
        n_member * RES_DEV, n_blocks, amp_hbm.shape[0], fetched.shape[0], count_ref[0], task_ref, slot_vmem, last_vmem,
    )
    slot_copy = pltpu.make_async_copy(slot_vmem, slot_ref, local_sem.at[5])
    last_copy = pltpu.make_async_copy(last_vmem, last_ref, local_sem.at[6])
    slot_copy.start()
    last_copy.start()
    amp_copy.wait()
    slot_copy.wait()
    last_copy.wait()
    for i in range(n_group - 1):
        asks[i].wait_send()
        source = (g + i + 1) % n_group
        pltpu.make_async_remote_copy(
            src_ref=outgoing.at[i], dst_ref=fetched.at[pl.ds(source * fetch_cap, fetch_cap)],
            send_sem=tile_send.at[i], recv_sem=tile_recv.at[i],
            device_id=group_peers[i], device_id_type=MESH,
        ).wait_recv()

    def block(b, total):
        for u in range(UNROLL):
            total = one_block(b * UNROLL + u, total)
        return total

    def one_block(b, total):
        left = []
        right = []
        for t in range(BLOCK):
            left.append(amps[slot_ref[0, b * BLOCK + t]])
            right.append(fetched[slot_ref[1, b * BLOCK + t]])
        product = jnp.dot(
            jnp.concatenate(left, axis=1), jnp.concatenate(right, axis=0), preferred_element_type=jnp.float32
        )
        total = jnp.where(slot_ref[2, b] != 0, total, 0.0) + product
        running[b] = total
        return total

    lax.fori_loop(0, n_blocks // UNROLL, block, jnp.zeros((tile, tile), jnp.float32))

    for k in range(n_z):
        half[k] = running[last_ref[2 * k + 1 - core, 0]]
    swap = pltpu.make_async_remote_copy(
        src_ref=half, dst_ref=half_in, send_sem=half_send, recv_sem=half_recv,
        device_id=sibling, device_id_type=MESH,
    )
    swap.start()
    swap.wait_recv()
    parts = []
    for i in range(1, n_z):
        k = (z + i) % n_z
        pair[i - 1] = running[last_ref[2 * k + core, 0]] + half_in[k]
        part = pltpu.make_async_remote_copy(
            src_ref=pair.at[i - 1], dst_ref=pair_in.at[i - 1],
            send_sem=pair_send.at[i - 1], recv_sem=pair_recv.at[i - 1],
            device_id=z_peers[i - 1], device_id_type=MESH,
        )
        part.start()
        parts.append(part)
    result = running[last_ref[m, 0]] + half_in[z]
    for i in range(n_z - 1):
        parts[i].wait_recv()
        result = result + pair_in[i]
    out_ref[0] = result
    swap.wait_send()
    for copy in sends + parts:
        copy.wait_send()


def sorted_tasks_call(amplitudes, integrals, tasks, requests, counts):
    tile = amplitudes.shape[1]
    n_group = lax.axis_size("group")
    n_member = lax.axis_size("member")
    n_res = RES_DEV * n_member
    cap = tasks.shape[0]
    fetch_cap = requests.shape[1]
    n_z = n_member // 2
    n_blocks = round_up((cap + BLOCK - 1) // BLOCK + n_res, UNROLL)
    slots = round_up(n_blocks * BLOCK, 128)
    vmem = pl.BlockSpec(memory_space=pltpu.VMEM)
    hbm = pl.BlockSpec(memory_space=pltpu.HBM)
    f32, bf16 = jnp.float32, amplitudes.dtype
    dma = pltpu.SemaphoreType.DMA
    return pl.pallas_call(
        functools.partial(main_kernel, n_group, n_member, n_blocks),
        out_shape=jax.ShapeDtypeStruct((RES_DEV, tile, tile), f32),
        in_specs=[hbm] * 5,
        out_specs=vmem,
        scratch_shapes=[
            pltpu.SMEM(requests.shape, jnp.int32),
            pltpu.VMEM((tasks.shape[1], cap), jnp.int32),
            pltpu.SMEM(counts.shape, jnp.int32),
            pltpu.VMEM((8, slots), jnp.int32),
            pltpu.VMEM((n_res, 128), jnp.int32),
            pltpu.SMEM((8, slots), jnp.int32),
            pltpu.SMEM((n_res, 128), jnp.int32),
            pltpu.VMEM((amplitudes.shape[0] + 1, tile, tile), bf16),
            pltpu.VMEM(integrals.shape, bf16),
            pltpu.VMEM((n_group * fetch_cap, tile, tile), bf16),
            pltpu.VMEM((n_group - 1, fetch_cap, tile, tile), bf16),
            pltpu.SMEM((n_group - 1,) + requests.shape, jnp.int32),
            pltpu.VMEM((n_blocks, tile, tile), f32),
            pltpu.VMEM((n_z, tile, tile), f32),
            pltpu.VMEM((n_z, tile, tile), f32),
            pltpu.VMEM((n_z - 1, tile, tile), f32),
            pltpu.VMEM((n_z - 1, tile, tile), f32),
            dma((7,)),
            dma((n_group - 1,)),
            dma((n_group - 1,)),
            dma((n_group - 1,)),
            dma((n_group - 1,)),
            dma,
            dma,
            dma((n_z - 1,)),
            dma((n_z - 1,)),
        ],
        compiler_params=pltpu.CompilerParams(
            collective_id=0, has_side_effects=True, vmem_limit_bytes=67043328
        ),
    )(requests, tasks.T, counts, amplitudes, integrals)


SUB = 8
CODES = 32767.0


def count_weights(n_bins, n_res, n_amps, parts, count, task_ref, e_ref, row_ref):
    cap = task_ref.shape[1]
    width = parts * n_amps * SUB
    share = -(-cap // parts)
    bins = task_ref[1:2, :] * n_res + task_ref[2:3, :]
    lane = lax.broadcasted_iota(jnp.int32, (1, cap), 1)
    amp = task_ref[0:1, :]
    for p in range(1, parts):
        amp = amp + jnp.where(lane >= p * share, n_amps, 0)
    hit_bin = (lax.broadcasted_iota(jnp.int32, (n_bins, cap), 0) == bins) & (
        lax.broadcasted_iota(jnp.int32, (n_bins, cap), 1) < count
    )
    first = amp * SUB
    rows = lax.broadcasted_iota(jnp.int32, (width, cap), 0)
    hit_amp = (rows >= first) & (rows < first + SUB)
    row_ref[...] = lax.dot_general(
        jnp.where(hit_bin, 1.0, 0.0).astype(jnp.bfloat16),
        jnp.where(hit_amp, 1.0, 0.0).astype(jnp.bfloat16),
        (((1,), (1,)), ((), ())),
        preferred_element_type=jnp.float32,
    )
    same = jnp.where(
        lax.broadcasted_iota(jnp.int32, (SUB, width), 1) % SUB
        == lax.broadcasted_iota(jnp.int32, (SUB, width), 0),
        1.0, 0.0,
    )
    for b in range(0, n_bins, 2):
        pair = [jnp.broadcast_to(row_ref[b + t:b + t + 1, :], (SUB, width)) * same for t in range(2)]
        e_ref[b * SUB:(b + 2) * SUB, :] = jnp.concatenate(pair, axis=0).astype(jnp.bfloat16)


def combine_amps(first, end, n_group, n_res, fetch_cap, parts, amps, e_ref, hi_ref, lo_ref):
    n_amps, tile = amps.shape[0], amps.shape[1]
    block = fetch_cap * n_res * SUB

    def rows16(q, carry):
        base = pl.multiple_of(q * 2 * SUB, 2 * SUB)
        rows = amps[:, pl.ds(base, 2 * SUB), :].astype(jnp.float32)
        halves = [
            rows[:, t * SUB:(t + 1) * SUB, :].reshape(n_amps * SUB, tile).astype(jnp.bfloat16) for t in range(2)
        ]
        right = jnp.concatenate(halves, axis=1)
        right = jnp.concatenate([right] * parts, axis=0)
        for h in range(n_group):
            made = jnp.dot(e_ref[h * block:(h + 1) * block, :], right, preferred_element_type=jnp.float32)
            for c in range(fetch_cap):
                for r in range(n_res):
                    at = (c * n_res + r) * SUB
                    value = jnp.concatenate(
                        [made[at:at + SUB, :tile], made[at:at + SUB, tile:]], axis=0
                    )
                    high = value.astype(jnp.bfloat16)
                    low = (value - high.astype(jnp.float32)).astype(jnp.bfloat16)
                    place = (h, pl.ds(pl.multiple_of(r * tile + base, 2 * SUB), 2 * SUB), pl.ds(c * tile, tile))
                    hi_ref[place] = high
                    lo_ref[place] = low
        return carry

    [rows16(q, 0) for q in range(first, end)]


def dense_kernel(
    n_group, n_member, parts,
    request_hbm, task_hbm, count_ref, amp_hbm, int_hbm, out_ref,
    request_ref, task_ref, amps, ints, fetched, outgoing, wanted, row_ref, e_ref, hi_ref, lo_ref, acc,
    half, half_in, code, code_in, scale, scale_in,
    local_sem, chain_sem, req_send, req_recv, tile_send, tile_recv, half_send, half_recv,
    code_send, code_recv, scale_send, scale_recv,
):
    g = lax.axis_index("group")
    m = lax.axis_index("member")
    n_z = n_member // 2
    n_res = n_member * RES_DEV
    z, core = m // 2, m % 2
    fetch_cap = request_ref.shape[1]
    tile = amps.shape[1]
    amp_copy = pltpu.make_async_copy(amp_hbm, amps, local_sem.at[0])
    int_copy = pltpu.make_async_copy(int_hbm, ints, local_sem.at[1])
    request_copy = pltpu.make_async_copy(request_hbm, request_ref, local_sem.at[2])
    task_copy = pltpu.make_async_copy(task_hbm, task_ref, local_sem.at[3])
    for copy in (request_copy, int_copy, task_copy, amp_copy):
        copy.start()
    row, col = g // 2, g % 2
    near = [row * 2 + 1 - col, (1 - row) * 2 + col]
    partners = near + [(1 - row) * 2 + 1 - col]
    sibling = (g, z * 2 + 1 - core)

    def to(i):
        return partners[i] if isinstance(i, int) else jnp.where(i == 0, partners[0], partners[1])


    barrier = pltpu.get_barrier_semaphore()

    def greet(device):
        pl.semaphore_signal(barrier, inc=1, device_id=device, device_id_type=MESH)

    for h in partners:
        greet((h, m))
    greet(sibling)

    @pl.when(z > 0)
    def _():
        greet((g, m - 2))

    @pl.when(z < n_z - 1)
    def _():
        greet((g, m + 2))

    request_copy.wait()
    ends = jnp.where(z > 0, 1, 0) + jnp.where(z < n_z - 1, 1, 0)
    pl.semaphore_wait(barrier, n_group + ends)

    def ask(i):
        return pltpu.make_async_remote_copy(
            src_ref=request_ref, dst_ref=wanted.at[i], send_sem=req_send.at[i], recv_sem=req_recv.at[i],
            device_id=(to(i), m), device_id_type=MESH,
        )

    def tiles(i, first=0, end=fetch_cap, slot=None):
        slot = i if slot is None else slot
        part = pl.ds(first, end - first)
        return pltpu.make_async_remote_copy(
            src_ref=outgoing.at[i, part], dst_ref=fetched.at[i + 1, part],
            send_sem=tile_send.at[slot], recv_sem=tile_recv.at[slot],
            device_id=(to(i), m), device_id_type=MESH,
        )

    far = n_group - 2
    split = fetch_cap // 2
    pieces = [tiles(i) for i in range(far)] + [tiles(far, 0, split), tiles(far, split, fetch_cap, far + 1)]

    ask(0).start()
    ask(1).start()
    ask(2).start()
    up, down = chain_sem.at[0], chain_sem.at[1]

    def tell_up():
        pl.semaphore_signal(up, inc=1, device_id=(g, m + 2), device_id_type=MESH)

    def tell_down():
        pl.semaphore_signal(down, inc=1, device_id=(g, m - 2), device_id_type=MESH)

    @pl.when((z == 1) & (z < n_z - 1))
    def _():
        tell_up()

    @pl.when((z == n_z - 2) & (z > 0))
    def _():
        tell_down()

    task_copy.wait()
    n_bins = n_group * fetch_cap * n_res
    count_weights(n_bins, n_res, amp_hbm.shape[0], parts, count_ref[0], task_ref, e_ref, row_ref)
    amp_copy.wait()
    steps = tile // (2 * SUB)
    early, middle = steps * 0 // 8, steps * 3 // 8

    def combine(first, end):
        combine_amps(first, end, n_group, n_res, fetch_cap, parts, amps, e_ref, hi_ref, lo_ref)

    combine(0, early)
    combine(early, middle)
    int_copy.wait()
    for c in range(fetch_cap):
        fetched[0, c] = ints[request_ref[g, c]]
    def serve(i, which):
        which.wait_recv()
        for c in range(fetch_cap):
            outgoing[i, c] = ints[wanted[i, g, c]]

    swapped = jnp.where((row == 1) & (col == 0), 1, 0)
    for i in (swapped, 1 - swapped):
        serve(i, ask(i))
        tiles(i).start()
    serve(far, ask(far))
    for piece in pieces[far:]:
        piece.start()

    combine(middle, steps)

    @pl.when((z > 1) & (z < n_z - 1))
    def _():
        pl.semaphore_wait(up, 1)
        tell_up()

    @pl.when((z < n_z - 2) & (z > 0))
    def _():
        pl.semaphore_wait(down, 1)
        tell_down()

    def product(i, r, first, end):
        h = g if i == 0 else partners[i - 1]
        place = (h, pl.ds(pl.multiple_of(r * tile, tile), tile), pl.ds(first * tile, (end - first) * tile))
        right = fetched[i, first:end].reshape((end - first) * tile, tile)
        return jnp.dot(hi_ref[place], right, preferred_element_type=jnp.float32) + jnp.dot(
            lo_ref[place], right, preferred_element_type=jnp.float32
        )

    for i in range(n_group - 1):
        if i > 0:
            pieces[i - 1].wait_recv()

        for r in range(n_res):
            value = product(i, r, 0, fetch_cap)
            acc[r] = value if i == 0 else acc[r] + value
    last = n_group - 1
    pieces[far].wait_recv()
    for r in range(n_res):
        acc[r] = acc[r] + product(last, r, 0, split)

    low_end = z < n_z // 2

    def order(t):
        down_v = n_z - 1 - t
        down_k = jnp.where(down_v > z, down_v, down_v - 1)
        up_k = jnp.where(t < z, t, t + 1)
        return jnp.where(low_end, down_k, up_k)

    def swap(k):
        return pltpu.make_async_remote_copy(
            src_ref=half.at[k], dst_ref=half_in.at[k], send_sem=half_send.at[k], recv_sem=half_recv.at[k],
            device_id=sibling, device_id_type=MESH,
        )

    ks = [order(t) for t in range(n_z - 1)] + [z]
    @pl.when((z > 1) & (z == n_z - 1))
    def _():
        pl.semaphore_wait(up, 1)

    @pl.when((z < n_z - 2) & (z == 0))
    def _():
        pl.semaphore_wait(down, 1)

    pieces[far + 1].wait_recv()
    for k in ks:
        r = 2 * k + 1 - core
        half[k] = acc[r] + product(last, r, split, fetch_cap)
    for k in ks:
        r = 2 * k + core
        acc[r] = acc[r] + product(last, r, split, fetch_cap)
    for k in ks:
        swap(k).start()

    def sends(k):
        return [
            pltpu.make_async_remote_copy(
                src_ref=s.at[k], dst_ref=d.at[z], send_sem=ss.at[k], recv_sem=rs.at[z],
                device_id=(g, 2 * k + core), device_id_type=MESH,
            )
            for s, d, ss, rs in (
                (scale, scale_in, scale_send, scale_recv), (code, code_in, code_send, code_recv),
            )
        ]

    def arrivals(k):
        return [
            pltpu.make_async_remote_copy(
                src_ref=s.at[k], dst_ref=d.at[k], send_sem=ss.at[k], recv_sem=rs.at[k],
                device_id=(g, 2 * k + core), device_id_type=MESH,
            )
            for s, d, ss, rs in (
                (scale, scale_in, scale_send, scale_recv), (code, code_in, code_send, code_recv),
            )
        ]

    for k in ks[:-1]:
        swap(k).wait_recv()
        value = acc[2 * k + core] + half_in[k]
        top = jnp.maximum(jnp.max(jnp.abs(value), axis=0, keepdims=True), 1e-30)
        scale[k] = top * (1.0 / CODES)
        code[k] = jnp.round(value * (CODES / top)).astype(jnp.int32).astype(jnp.int16)
        for copy in sends(k):
            copy.start()
    swap(z).wait_recv()
    result = acc[m] + half_in[z]
    for k in reversed(ks[:-1]):
        for copy in arrivals(k):
            copy.wait_recv()
        part = code_in[k].astype(jnp.int32).astype(jnp.float32)
        result = result + part * scale_in[k]
    out_ref[0] = result
    for i in range(n_group - 1):
        ask(i).wait_send()
    for piece in pieces:
        piece.wait_send()
    for k in ks:
        swap(k).wait_send()
    for k in ks[:-1]:
        for copy in sends(k):
            copy.wait_send()


def dense_call(amplitudes, integrals, tasks, requests, counts):
    n_amps, tile = amplitudes.shape[0], amplitudes.shape[1]
    pin = functools.partial(pltpu.with_memory_space_constraint, memory_space=pltpu.HBM)
    n_group = lax.axis_size("group")
    n_member = lax.axis_size("member")
    n_res = RES_DEV * n_member
    n_z = n_member // 2
    cap = tasks.shape[0]
    fetch_cap = requests.shape[1]
    n_bins = n_group * fetch_cap * n_res
    parts = -(-cap // 256)
    width = parts * n_amps * SUB
    vmem = pl.BlockSpec(memory_space=pltpu.VMEM)
    hbm = pl.BlockSpec(memory_space=pltpu.HBM)
    f32, bf16 = jnp.float32, amplitudes.dtype
    dma = pltpu.SemaphoreType.DMA
    return pl.pallas_call(
        functools.partial(dense_kernel, n_group, n_member, parts),
        out_shape=jax.ShapeDtypeStruct((RES_DEV, tile, tile), f32),
        in_specs=[hbm, hbm, pl.BlockSpec(memory_space=pltpu.SMEM), hbm, hbm],
        out_specs=vmem,
        scratch_shapes=[
            pltpu.SMEM(requests.shape, jnp.int32),
            pltpu.VMEM((tasks.shape[1], cap), jnp.int32),
            pltpu.VMEM(amplitudes.shape, bf16),
            pltpu.VMEM(integrals.shape, bf16),
            pltpu.VMEM((n_group, fetch_cap, tile, tile), bf16),
            pltpu.VMEM((n_group - 1, fetch_cap, tile, tile), bf16),
            pltpu.SMEM((n_group - 1,) + requests.shape, jnp.int32),
            pltpu.VMEM((n_bins, width), f32),
            pltpu.VMEM((n_bins * SUB, width), bf16),
            pltpu.VMEM((n_group, n_res * tile, fetch_cap * tile), bf16),
            pltpu.VMEM((n_group, n_res * tile, fetch_cap * tile), bf16),
            pltpu.VMEM((n_res, tile, tile), f32),
            pltpu.VMEM((n_z, tile, tile), f32),
            pltpu.VMEM((n_z, tile, tile), f32),
            pltpu.VMEM((n_z, tile, tile), jnp.int16),
            pltpu.VMEM((n_z, tile, tile), jnp.int16),
            pltpu.VMEM((n_z, 1, tile), f32),
            pltpu.VMEM((n_z, 1, tile), f32),
            dma((5,)),
            pltpu.SemaphoreType.REGULAR((2,)),
            dma((n_group - 1,)),
            dma((n_group - 1,)),
            dma((n_group,)),
            dma((n_group,)),
            dma((n_z,)),
            dma((n_z,)),
            dma((n_z,)),
            dma((n_z,)),
            dma((n_z,)),
            dma((n_z,)),
        ],
        compiler_params=pltpu.CompilerParams(
            collective_id=0, has_side_effects=True, vmem_limit_bytes=50331648
        ),
    )(pin(requests), pin(tasks.T), counts, pin(amplitudes), pin(integrals))


def per_device(amplitudes, integrals, tasks, requests, counts):
    n_bins = lax.axis_size("group") * requests.shape[1] * lax.axis_size("member") * RES_DEV
    if lax.axis_size("group") == 4 and n_bins * 2 <= tasks.shape[0]:
        return dense_call(amplitudes, integrals, tasks, requests, counts)
    return sorted_tasks_call(amplitudes, integrals, tasks, requests, counts)


def solution(mesh):
    return jax.shard_map(
        per_device,
        mesh=mesh,
        in_specs=(
            P(("group", "member"), None, None),
            P(("group", "member"), None, None),
            P(("group", "member"), None),
            P(("group", "member"), None),
            P(("group", "member")),
        ),
        out_specs=P(("group", "member"), None, None),
        check_vma=False,
    )
```
